8 devices in a mesh: dp: 2 (over z, y), tp: 4 (over x, core).
Axes of the slice: x: 2, y: 2, z: 1, core: 2. Of those that a mesh axis runs over, the one named last changes fastest.
Arguments:
- token_ids: int32 [8192], P('dp'), parts along dimension 0
- embed_table: bfloat16 [256000, 2048], P('tp')
- norm_gain: bfloat16 [2048], replicated
- w_in: bfloat16 [2048, 16384], P(None, 'tp')
- w_out: bfloat16 [16384, 2048], P('tp')
Outputs:
- output: bfloat16 [8192, 2048], P(('dp', 'tp')), parts along dimension 0
There are 2 independent parts. The reference program is written for one: setup_inputs(seed, part) draws one part's arguments, and reference() takes and returns one part's arrays. A program takes and returns all parts, laid end to end along the dimension named above; an argument that names none is the same for every part.
All inputs are finite; a program needn't handle non-finite values.
Results may differ from the reference program's by a relative error of at most 0.001.
Values are sent between devices in bfloat16 or wider.
A program may use at most 1.25 GiB of HBM per device.

```python
import math
import jax
import jax.numpy as jnp
from jax import lax

TOKENS = 4096
VOCAB_SIZE = 256000
MODEL_DIM = 2048
MLP_WIDTH = 16384
RMS_EPS = 1e-6
ROW_BLOCK = math.gcd(TOKENS, 256)


def draw_token_ids(key):
    key_mix, key_low, key_all, key_first, key_last = jax.random.split(key, 5)
    choose_low = jax.random.randint(key_mix, (TOKENS,), 0, 4) == 0
    low_ids = jax.random.randint(key_low, (TOKENS,), 0, VOCAB_SIZE // 8)
    any_ids = jax.random.randint(key_all, (TOKENS,), 0, VOCAB_SIZE)
    token_ids = jnp.where(choose_low, low_ids, any_ids)
    first_pos = jax.random.randint(key_first, (), 0, TOKENS // 2)
    last_pos = jax.random.randint(key_last, (), TOKENS // 2, TOKENS)
    token_ids = token_ids.at[first_pos].set(0).at[last_pos].set(VOCAB_SIZE - 1)
    return token_ids.astype(jnp.int32)


def setup_inputs(seed: int = 0, part: int = 0) -> dict:
    base_key = jax.random.key(seed)
    key_ids = jax.random.fold_in(jax.random.fold_in(base_key, 1), part)
    key_table, key_gain, key_in, key_out = jax.random.split(jax.random.fold_in(base_key, 2), 4)
    embed_table = jax.random.normal(key_table, (VOCAB_SIZE, MODEL_DIM), jnp.float32)
    norm_gain = jax.random.uniform(key_gain, (MODEL_DIM,), jnp.float32, 0.5, 1.5)
    w_in = jax.random.normal(key_in, (MODEL_DIM, MLP_WIDTH), jnp.float32) * MODEL_DIM ** -0.5
    w_out = jax.random.normal(key_out, (MLP_WIDTH, MODEL_DIM), jnp.float32) * MLP_WIDTH ** -0.5
    return {
        "token_ids": draw_token_ids(key_ids),
        "embed_table": embed_table.astype(jnp.bfloat16),
        "norm_gain": norm_gain.astype(jnp.bfloat16),
        "w_in": w_in.astype(jnp.bfloat16),
        "w_out": w_out.astype(jnp.bfloat16),
    }


def block_forward(embed_rows, norm_gain, w_in, w_out):
    rows_f32 = embed_rows.astype(jnp.float32)
    inv_rms = lax.rsqrt(jnp.mean(rows_f32 * rows_f32, axis=-1, keepdims=True) + RMS_EPS)
    normed = (rows_f32 * inv_rms * norm_gain.astype(jnp.float32)).astype(jnp.bfloat16)
    pre_act = jnp.dot(normed, w_in, preferred_element_type=jnp.float32).astype(jnp.bfloat16)
    activated = jax.nn.gelu(pre_act.astype(jnp.float32), approximate=True).astype(jnp.bfloat16)
    mlp_sum = jnp.dot(activated, w_out, preferred_element_type=jnp.float32)
    return (rows_f32 + mlp_sum).astype(jnp.bfloat16)


def reference(token_ids, embed_table, norm_gain, w_in, w_out):
    embedded = jnp.take(embed_table, token_ids, axis=0)
    row_blocks = embedded.reshape(TOKENS // ROW_BLOCK, ROW_BLOCK, MODEL_DIM)
    outputs = lax.map(lambda row_blk: block_forward(row_blk, norm_gain, w_in, w_out), row_blocks)
    return outputs.reshape(TOKENS, MODEL_DIM)
```

```python
import functools

import jax
import jax.numpy as jnp
from jax import lax
from jax.experimental import pallas as pl
from jax.experimental.pallas import tpu as pltpu
from jax.sharding import PartitionSpec as P

RMS_EPS = 1e-6
TILE = 32
SLOTS = 6
PIECE = 128
CHUNK = 512
WIDTH = 512
MESH = pl.DeviceIdType.MESH


def gather_kernel(tiles, span_ref, ids_ref, pick_ref, table_ref, out_ref, slabs, rows, steps, slab_sem, row_sem):
    n_spans = span_ref.shape[0] // 2
    total = 0
    for span in range(n_spans):
        first, last = span_ref[2 * span], span_ref[2 * span + 1]

        def note(t, _, span=span, first=first, total=total):
            steps[total + t - first] = span * tiles + t
            return 0

        lax.fori_loop(first, last, note, 0)
        total = total + last - first

    def fetch(step):
        slot = lax.rem(step, SLOTS)
        base = steps[step] * TILE
        for j in range(TILE):
            slab = lax.shift_right_logical(ids_ref[base + j], 3)
            pltpu.make_async_copy(
                table_ref.at[slab], slabs.at[slot, pl.ds(8 * j, 8), :], slab_sem.at[slot]
            ).start()

    for step in range(SLOTS - 1):
        @pl.when(step < total)
        def _(step=step):
            fetch(step)

    def out_copy(step):
        slot = lax.rem(step, 2)
        return pltpu.make_async_copy(
            rows.at[slot], out_ref.at[pl.ds(steps[step] * TILE, TILE), :], row_sem.at[slot]
        )

    def work(step, _):
        @pl.when(step + SLOTS - 1 < total)
        def _():
            fetch(step + SLOTS - 1)

        slot = lax.rem(step, SLOTS)
        pltpu.make_async_copy(slabs.at[slot], slabs.at[slot], slab_sem.at[slot]).wait()
        base = pl.multiple_of(steps[step] * TILE, TILE)
        col = lax.broadcasted_iota(jnp.int32, (TILE, 8 * TILE), 1)
        want = pick_ref[pl.ds(base, TILE), :] + 8 * lax.broadcasted_iota(jnp.int32, (TILE, 8 * TILE), 0)
        pick = (col == want).astype(jnp.float32).astype(jnp.bfloat16)

        @pl.when(step >= 2)
        def _():
            out_copy(step - 2).wait()

        rows[lax.rem(step, 2)] = jnp.dot(
            pick, slabs[slot], preferred_element_type=jnp.float32
        ).astype(jnp.bfloat16)
        out_copy(step).start()
        return 0

    lax.fori_loop(0, total, work, 0)
    for back in (2, 1):
        @pl.when(total >= back)
        def _(back=back):
            out_copy(total - back).wait()


def gather_rows(table_shard, spans, ids, picks, cap):
    n_rows, dim = ids.shape[0], table_shard.shape[1]
    return pl.pallas_call(
        functools.partial(gather_kernel, cap // TILE),
        out_shape=jax.ShapeDtypeStruct((n_rows, dim), jnp.bfloat16),
        in_specs=[
            pl.BlockSpec(memory_space=pltpu.SMEM),
            pl.BlockSpec(memory_space=pltpu.SMEM),
            pl.BlockSpec(memory_space=pltpu.VMEM),
            pl.BlockSpec(memory_space=pl.ANY),
        ],
        out_specs=pl.BlockSpec(memory_space=pl.ANY),
        scratch_shapes=[
            pltpu.VMEM((SLOTS, 8 * TILE, dim), jnp.bfloat16),
            pltpu.VMEM((2, TILE, dim), jnp.bfloat16),
            pltpu.SMEM((n_rows // TILE,), jnp.int32),
            pltpu.SemaphoreType.DMA((SLOTS,)),
            pltpu.SemaphoreType.DMA((2,)),
        ],
        compiler_params=pltpu.CompilerParams(vmem_limit_bytes=40 << 20),
        name="gather_rows",
    )(spans, ids, picks, table_shard.reshape(-1, 8, dim))


def prepare(token_ids, shard_rows, cap):
    me = lax.axis_index("tp")
    chip = me // 2
    other, partner = me ^ 2, me ^ 1
    blocks = jnp.stack([other ^ 1, partner, other, me])
    ids = jnp.take(token_ids.reshape(4, -1), blocks, axis=0)
    n_tok = ids.shape[1]
    owner = ids // shard_rows
    is_of = (owner[:, None, :] == jnp.arange(4)[None, :, None])
    upto = (lax.broadcasted_iota(jnp.int32, (n_tok, n_tok), 0) <= lax.broadcasted_iota(jnp.int32, (n_tok, n_tok), 1))
    counts_to = jnp.dot(
        is_of.reshape(16, n_tok).astype(jnp.bfloat16), upto.astype(jnp.bfloat16), preferred_element_type=jnp.float32
    ).astype(jnp.int32).reshape(4, 4, n_tok)
    counts = counts_to[:, :, -1]
    starts = jnp.stack([jnp.zeros_like(counts[:, 0]), counts[:, 0], jnp.zeros_like(counts[:, 0]), counts[:, 2]], axis=1)
    place = jnp.sum(jnp.where(is_of, counts_to - 1 + starts[:, :, None], 0), axis=1)

    my_start = jnp.take(starts, me, axis=1)
    my_end = my_start + jnp.take(counts, me, axis=1)
    spans = jnp.stack([my_start // TILE, (my_end + TILE - 1) // TILE], axis=1)
    spans = jnp.where((my_end > my_start)[:, None], spans, 0).reshape(8)
    mine = owner == me
    slot = lax.broadcasted_iota(jnp.int32, (4, n_tok, cap), 2)
    hit = (place[:, :, None] == slot) & mine[:, :, None]
    ids_at = jnp.max(jnp.where(hit, (ids - me * shard_rows)[:, :, None], 0), axis=1).reshape(-1)
    picks = (ids_at & 7)[:, None]

    ours = (owner // 2) == chip
    from_ours = jnp.where(ours, place, -1)[2:, :, None]
    from_other = jnp.where(ours, -1, place)[2:, :, None]
    first = jnp.take(counts, 2 * chip, axis=1)[2:, None]
    both = first + jnp.take(counts, 2 * chip + 1, axis=1)[2:, None]
    pos = lax.broadcasted_iota(jnp.int32, (2, cap), 1)
    is_core0 = pos < first
    source = jnp.where(pos < both, jnp.where(is_core0 == (me % 2 == 0), 0, 1), 2)[:, :, None]
    return spans, ids_at, picks, from_ours, from_other, source


def block_kernel(
    cap, gain_ref, ours_ref, other_ref, source_ref, rows_ref, w1_ref, w2_ref,
    out_ref, w1p_ref, w2p_ref, sums_ref,
    inbox, ours_rows, normed, kept, acc, w1_buf, w2_buf, sum_buf, out_buf,
    pair_send, pair_recv, load_sem, w_send, w_recv, ready, x_send, x_recv, w_sem, s_send, s_recv, r_sem, o_sem,
):
    me, dp = lax.axis_index("tp"), lax.axis_index("dp")
    core = lax.rem(me, 2)
    partner = me + 1 - 2 * core
    other = lax.rem(me + 2, 4)
    dim = gain_ref.shape[1]
    n_tok = out_ref.shape[0]
    width = w1_ref.shape[1]
    w_steps = width // WIDTH
    n_chunks = n_tok // CHUNK
    n_pieces = n_tok // PIECE

    barrier = pltpu.get_barrier_semaphore()
    for peer in (partner, other):
        pl.semaphore_signal(barrier, inc=1, device_id=(dp, peer), device_id_type=MESH)
    pl.semaphore_wait(barrier, 2)

    def remote(src, dst, send, recv, peer):
        return pltpu.make_async_remote_copy(
            src_ref=src, dst_ref=dst, send_sem=send, recv_sem=recv, device_id=(dp, peer), device_id_type=MESH
        )

    pair = [
        remote(rows_ref.at[pl.ds((1 - p) * cap, cap), :], inbox.at[p], pair_send.at[p], pair_recv.at[p], partner)
        for p in range(2)
    ]
    loads = [
        pltpu.make_async_copy(rows_ref.at[pl.ds((3 - p) * cap, cap), :], ours_rows.at[1 - p], load_sem.at[p])
        for p in range(2)
    ]
    weights = [
        remote(w1_ref, w1p_ref, w_send.at[0], w_recv.at[0], partner),
        remote(w2_ref, w2p_ref, w_send.at[1], w_recv.at[1], partner),
    ]
    for p in range(2):
        pair[p].start()
        loads[p].start()
    for copy in weights:
        copy.start()

    def fetch_weights(step, slot, start):
        @pl.when(step < w_steps)
        def _():
            cols = pl.ds(pl.multiple_of(step * WIDTH, WIDTH), WIDTH)
            start(pltpu.make_async_copy(w1_ref.at[:, cols], w1_buf.at[slot], w_sem.at[0, slot]))
            start(pltpu.make_async_copy(w2_ref.at[cols, :], w2_buf.at[slot], w_sem.at[1, slot]))

        @pl.when(step >= w_steps)
        def _():
            cols = pl.ds(pl.multiple_of((step - w_steps) * WIDTH, WIDTH), WIDTH)
            start(pltpu.make_async_copy(w1p_ref.at[:, cols], w1_buf.at[slot], w_sem.at[0, slot]))
            start(pltpu.make_async_copy(w2p_ref.at[cols, :], w2_buf.at[slot], w_sem.at[1, slot]))

    fetch_weights(0, 0, lambda copy: copy.start())

    cross = [
        remote(ours_rows.at[1 - p], inbox.at[p], x_send.at[p], x_recv.at[p], other) for p in range(2)
    ]
    for p in range(2):
        b = 1 - p
        loads[p].wait()
        pair[p].wait_recv()

        @pl.loop(0, cap // TILE)
        def _(t, p=p, b=b):
            span = pl.ds(pl.multiple_of(t * TILE, TILE), TILE)
            source = source_ref[b, span, :]
            mine = ours_rows[b, span, :].astype(jnp.float32)
            theirs = inbox[p, span, :].astype(jnp.float32)
            ours_rows[b, span, :] = jnp.where(
                source == 0, mine, jnp.where(source == 1, theirs, 0.0)
            ).astype(jnp.bfloat16)

        pl.semaphore_signal(ready.at[p], inc=1, device_id=(dp, other), device_id_type=MESH)
        pl.semaphore_wait(ready.at[p], 1)
        cross[p].start()

    gain = gain_ref[...].astype(jnp.float32)

    def send_sums(piece):
        span = pl.ds(pl.multiple_of(piece * PIECE, PIECE), PIECE)
        return remote(acc.at[span, :], sums_ref.at[span, :], s_send.at[piece], s_recv.at[piece], other)

    @pl.loop(0, 2)
    def _(b):
        remote(ours_rows.at[b], inbox.at[b], x_send.at[b], x_recv.at[b], other).wait_recv()

        @pl.loop(0, n_tok // 256)
        def _(t):
            span = pl.ds(pl.multiple_of(t * 256, 256), 256)
            slot = lax.broadcasted_iota(jnp.int32, (256, cap), 1)
            pick_ours = (slot == ours_ref[b, span, :]).astype(jnp.float32).astype(jnp.bfloat16)
            pick_other = (slot == other_ref[b, span, :]).astype(jnp.float32).astype(jnp.bfloat16)
            rows = jnp.dot(pick_ours, ours_rows[b], preferred_element_type=jnp.float32) + jnp.dot(
                pick_other, inbox[b], preferred_element_type=jnp.float32
            )
            kept[span, :] = rows.astype(jnp.bfloat16)
            inv_rms = lax.rsqrt(jnp.mean(rows * rows, axis=-1, keepdims=True) + RMS_EPS)
            normed[span, :] = (rows * inv_rms * gain).astype(jnp.bfloat16)

        @pl.loop(0, n_chunks)
        def _(chunk):
            tok = pl.ds(pl.multiple_of(chunk * CHUNK, CHUNK), CHUNK)
            out_rows = pl.ds(pl.multiple_of(b * n_tok + chunk * CHUNK, CHUNK), CHUNK)
            acc[out_rows, :] = jnp.zeros((CHUNK, dim), jnp.float32)

            @pl.loop(0, 2 * w_steps)
            def _(w):
                step = (b * n_chunks + chunk) * 2 * w_steps + w
                slot = lax.rem(step, 2)
                fetch_weights(w, slot, lambda copy: copy.wait())

                @pl.when(step == w_steps - 1)
                def _():
                    for copy in weights:
                        copy.wait_recv()

                @pl.when(step + 1 < 2 * n_chunks * 2 * w_steps)
                def _():
                    fetch_weights(lax.rem(step + 1, 2 * w_steps), 1 - slot, lambda copy: copy.start())

                parts = []
                for half in range(2):
                    cols = pl.ds(half * (WIDTH // 2), WIDTH // 2)
                    z = jnp.dot(normed[tok, :], w1_buf[slot, :, cols], preferred_element_type=jnp.float32)
                    z = z.astype(jnp.bfloat16).astype(jnp.float32)
                    inner = 0.7978845608028654 * (z + 0.044715 * (z * z * z))
                    parts.append((0.5 * z * (1.0 + jnp.tanh(inner))).astype(jnp.bfloat16))
                hidden = jnp.concatenate(parts, axis=1)
                for half in range(2):
                    cols = pl.ds(half * (dim // 2), dim // 2)
                    acc[out_rows, cols] += jnp.dot(
                        hidden, w2_buf[slot, :, cols], preferred_element_type=jnp.float32
                    )

            @pl.when(b == 0)
            def _():
                for q in range(CHUNK // PIECE):
                    send_sums(chunk * (CHUNK // PIECE) + q).start()

    def take_sums(piece, slot):
        span = pl.ds(pl.multiple_of(piece * PIECE, PIECE), PIECE)
        return pltpu.make_async_copy(sums_ref.at[span, :], sum_buf.at[slot], r_sem.at[slot])

    def put_out(piece, slot):
        span = pl.ds(pl.multiple_of(piece * PIECE, PIECE), PIECE)
        return pltpu.make_async_copy(out_buf.at[slot], out_ref.at[span, :], o_sem.at[slot])

    @pl.loop(0, n_pieces)
    def _(piece):
        slot = lax.rem(piece, 2)
        send_sums(piece).wait_recv()
        take = take_sums(piece, slot)
        take.start()
        take.wait()

        @pl.when(piece >= 2)
        def _():
            put_out(piece - 2, slot).wait()

        span = pl.ds(pl.multiple_of(piece * PIECE, PIECE), PIECE)
        own = pl.ds(pl.multiple_of(n_tok + piece * PIECE, PIECE), PIECE)
        total = acc[own, :] + sum_buf[slot]
        out_buf[slot] = (kept[span, :].astype(jnp.float32) + total).astype(jnp.bfloat16)
        put_out(piece, slot).start()

    put_out(n_pieces - 2, lax.rem(n_pieces - 2, 2)).wait()
    put_out(n_pieces - 1, lax.rem(n_pieces - 1, 2)).wait()

    for copy in pair + weights + cross:
        copy.wait_send()

    @pl.loop(0, n_pieces)
    def _(piece):
        send_sums(piece).wait_send()


def mlp_block(gain, from_ours, from_other, source, rows, w_in, w_out, n_tok, cap):
    dim, width = w_in.shape
    any_spec, vmem = pl.BlockSpec(memory_space=pl.ANY), pl.BlockSpec(memory_space=pltpu.VMEM)
    dma = pltpu.SemaphoreType.DMA
    n_pieces = n_tok // PIECE
    flops = 2 * (2 * n_tok) * dim * (2 * width) * 2
    return pl.pallas_call(
        functools.partial(block_kernel, cap),
        out_shape=[
            jax.ShapeDtypeStruct((n_tok, dim), jnp.bfloat16),
            jax.ShapeDtypeStruct(w_in.shape, w_in.dtype),
            jax.ShapeDtypeStruct(w_out.shape, w_out.dtype),
            jax.ShapeDtypeStruct((n_tok, dim), jnp.float32),
        ],
        in_specs=[vmem, vmem, vmem, vmem, any_spec, any_spec, any_spec],
        out_specs=[any_spec] * 4,
        scratch_shapes=[
            pltpu.VMEM((2, cap, dim), jnp.bfloat16),
            pltpu.VMEM((2, cap, dim), jnp.bfloat16),
            pltpu.VMEM((n_tok, dim), jnp.bfloat16),
            pltpu.VMEM((n_tok, dim), jnp.bfloat16),
            pltpu.VMEM((2 * n_tok, dim), jnp.float32),
            pltpu.VMEM((2, dim, WIDTH), jnp.bfloat16),
            pltpu.VMEM((2, WIDTH, dim), jnp.bfloat16),
            pltpu.VMEM((2, PIECE, dim), jnp.float32),
            pltpu.VMEM((2, PIECE, dim), jnp.bfloat16),
            dma((2,)), dma((2,)), dma((2,)), dma((2,)), dma((2,)),
            pltpu.SemaphoreType.REGULAR((2,)),
            dma((2,)), dma((2,)), dma((2, 2)), dma((n_pieces,)), dma((n_pieces,)), dma((2,)), dma((2,)),
        ],
        compiler_params=pltpu.CompilerParams(
            collective_id=0, has_side_effects=True, vmem_limit_bytes=67043328
        ),
        cost_estimate=pl.CostEstimate(flops=flops, bytes_accessed=1 << 28, transcendentals=0),
        name="mlp_block",
    )(gain, from_ours, from_other, source, rows, w_in, w_out)


def solution(mesh):
    def device_step(token_ids, table_shard, norm_gain, w_in_shard, w_out_shard):
        n_tok = token_ids.shape[0] // 4
        cap = n_tok
        spans, ids_at, picks, from_ours, from_other, source = prepare(token_ids, table_shard.shape[0], cap)
        rows = gather_rows(table_shard, spans, ids_at, picks, cap)
        return mlp_block(
            norm_gain[None, :], from_ours, from_other, source, rows, w_in_shard, w_out_shard, n_tok, cap
        )[0]

    return jax.shard_map(
        device_step,
        mesh=mesh,
        in_specs=(P("dp"), P("tp", None), P(), P(None, "tp"), P("tp", None)),
        out_specs=P(("dp", "tp"), None),
        check_vma=False,
    )
```

```python
import functools

import jax
import jax.numpy as jnp
from jax import lax
from jax.experimental import pallas as pl
from jax.experimental.pallas import tpu as pltpu
from jax.sharding import PartitionSpec as P

RMS_EPS = 1e-6
TILE = 32
SLOTS = 6
PIECE = 128
CHUNK = 512
WIDTH = 512
PACKED = 704
MESH = pl.DeviceIdType.MESH


def gather_kernel(tiles, span_ref, ids_ref, pick_ref, table_ref, out_ref, slabs, rows, steps, slab_sem, row_sem):
    n_spans = span_ref.shape[0] // 2
    total = 0
    for span in range(n_spans):
        first, last = span_ref[2 * span], span_ref[2 * span + 1]

        def note(t, _, span=span, first=first, total=total):
            steps[total + t - first] = span * tiles + t
            return 0

        lax.fori_loop(first, last, note, 0)
        total = total + last - first

    def fetch(step):
        slot = lax.rem(step, SLOTS)
        base = steps[step] * TILE
        for j in range(TILE):
            slab = lax.shift_right_logical(ids_ref[base + j], 3)
            pltpu.make_async_copy(
                table_ref.at[slab], slabs.at[slot, pl.ds(8 * j, 8), :], slab_sem.at[slot]
            ).start()

    for step in range(SLOTS - 1):
        @pl.when(step < total)
        def _(step=step):
            fetch(step)

    def out_copy(step):
        slot = lax.rem(step, 2)
        return pltpu.make_async_copy(
            rows.at[slot], out_ref.at[pl.ds(steps[step] * TILE, TILE), :], row_sem.at[slot]
        )

    def work(step, _):
        @pl.when(step + SLOTS - 1 < total)
        def _():
            fetch(step + SLOTS - 1)

        slot = lax.rem(step, SLOTS)
        pltpu.make_async_copy(slabs.at[slot], slabs.at[slot], slab_sem.at[slot]).wait()
        base = pl.multiple_of(steps[step] * TILE, TILE)
        col = lax.broadcasted_iota(jnp.int32, (TILE, 8 * TILE), 1)
        want = pick_ref[pl.ds(base, TILE), :] + 8 * lax.broadcasted_iota(jnp.int32, (TILE, 8 * TILE), 0)
        pick = (col == want).astype(jnp.float32).astype(jnp.bfloat16)

        @pl.when(step >= 2)
        def _():
            out_copy(step - 2).wait()

        rows[lax.rem(step, 2)] = jnp.dot(
            pick, slabs[slot], preferred_element_type=jnp.float32
        ).astype(jnp.bfloat16)
        out_copy(step).start()
        return 0

    lax.fori_loop(0, total, work, 0)
    for back in (2, 1):
        @pl.when(total >= back)
        def _(back=back):
            out_copy(total - back).wait()


def gather_rows(table_shard, spans, ids, picks, cap):
    n_rows, dim = ids.shape[0], table_shard.shape[1]
    return pl.pallas_call(
        functools.partial(gather_kernel, cap // TILE),
        out_shape=jax.ShapeDtypeStruct((n_rows, dim), jnp.bfloat16),
        in_specs=[
            pl.BlockSpec(memory_space=pltpu.SMEM),
            pl.BlockSpec(memory_space=pltpu.SMEM),
            pl.BlockSpec(memory_space=pltpu.VMEM),
            pl.BlockSpec(memory_space=pl.ANY),
        ],
        out_specs=pl.BlockSpec(memory_space=pl.ANY),
        scratch_shapes=[
            pltpu.VMEM((SLOTS, 8 * TILE, dim), jnp.bfloat16),
            pltpu.VMEM((2, TILE, dim), jnp.bfloat16),
            pltpu.SMEM((n_rows // TILE,), jnp.int32),
            pltpu.SemaphoreType.DMA((SLOTS,)),
            pltpu.SemaphoreType.DMA((2,)),
        ],
        compiler_params=pltpu.CompilerParams(vmem_limit_bytes=40 << 20),
        cost_estimate=pl.CostEstimate(flops=1 << 34, bytes_accessed=1 << 26, transcendentals=0),
        name="gather_rows",
    )(spans, ids, picks, table_shard.reshape(-1, 8, dim))


def prepare(token_ids, shard_rows, cap):
    me = lax.axis_index("tp")
    chip = me // 2
    other, partner = me ^ 2, me ^ 1
    blocks = jnp.stack([other ^ 1, partner, other, me])
    ids = jnp.take(token_ids.reshape(4, -1), blocks, axis=0)
    n_tok = ids.shape[1]
    owner = ids // shard_rows
    is_of = (owner[:, None, :] == jnp.arange(4)[None, :, None])
    upto = (lax.broadcasted_iota(jnp.int32, (n_tok, n_tok), 0) <= lax.broadcasted_iota(jnp.int32, (n_tok, n_tok), 1))
    counts_to = jnp.dot(
        is_of.reshape(16, n_tok).astype(jnp.bfloat16), upto.astype(jnp.bfloat16), preferred_element_type=jnp.float32
    ).astype(jnp.int32).reshape(4, 4, n_tok)
    counts = counts_to[:, :, -1]
    starts = jnp.stack([jnp.zeros_like(counts[:, 0]), counts[:, 0], jnp.zeros_like(counts[:, 0]), counts[:, 2]], axis=1)
    place = jnp.sum(jnp.where(is_of, counts_to - 1 + starts[:, :, None], 0), axis=1)

    my_start = jnp.take(starts, me, axis=1)
    my_end = my_start + jnp.take(counts, me, axis=1)
    spans = jnp.stack([my_start // TILE, (my_end + TILE - 1) // TILE], axis=1)
    spans = jnp.where((my_end > my_start)[:, None], spans, 0).reshape(8)
    mine = owner == me
    slot = lax.broadcasted_iota(jnp.int32, (4, n_tok, cap), 2)
    hit = (place[:, :, None] == slot) & mine[:, :, None]
    ids_at = jnp.max(jnp.where(hit, (ids - me * shard_rows)[:, :, None], 0), axis=1).reshape(-1)
    picks = (ids_at & 7)[:, None]

    ours = (owner // 2) == chip
    from_ours = jnp.where(ours, place, -1)[2:, :, None]
    from_other = jnp.where(ours, -1, place)[2:, :, None]
    first = jnp.take(counts, 2 * chip, axis=1)[2:, None]
    both = first + jnp.take(counts, 2 * chip + 1, axis=1)[2:, None]
    pos = lax.broadcasted_iota(jnp.int32, (2, cap), 1)
    is_core0 = pos < first
    source = jnp.where(pos < both, jnp.where(is_core0 == (me % 2 == 0), 0, 1), 2)[:, :, None]
    most = jnp.max(jnp.stack([counts[:, 0] + counts[:, 1], counts[:, 2] + counts[:, 3]]))
    return spans, ids_at, picks, from_ours, from_other, source, most


def block_kernel(
    cap, stride, gain_ref, ours_ref, other_ref, source_ref, rows_ref, w1_ref, w2_ref,
    out_ref, w1p_ref, w2p_ref, sums_ref,
    inbox, ours_rows, normed, kept, acc, w1_buf, w2_buf, sum_buf, out_buf,
    pair_send, pair_recv, load_sem, w_send, w_recv, ready, x_send, x_recv, w_sem, s_send, s_recv, r_sem, o_sem,
):
    me, dp = lax.axis_index("tp"), lax.axis_index("dp")
    core = lax.rem(me, 2)
    partner = me + 1 - 2 * core
    other = lax.rem(me + 2, 4)
    dim = gain_ref.shape[1]
    n_tok = out_ref.shape[0]
    width = w1_ref.shape[1]
    w_steps = width // WIDTH
    n_chunks = n_tok // CHUNK
    n_pieces = n_tok // PIECE

    barrier = pltpu.get_barrier_semaphore()
    for peer in (partner, other):
        pl.semaphore_signal(barrier, inc=1, device_id=(dp, peer), device_id_type=MESH)
    pl.semaphore_wait(barrier, 2)

    def remote(src, dst, send, recv, peer):
        return pltpu.make_async_remote_copy(
            src_ref=src, dst_ref=dst, send_sem=send, recv_sem=recv, device_id=(dp, peer), device_id_type=MESH
        )

    pair = [
        remote(rows_ref.at[pl.ds((1 - p) * stride, cap), :], inbox.at[p], pair_send.at[p], pair_recv.at[p], partner)
        for p in range(2)
    ]
    loads = [
        pltpu.make_async_copy(rows_ref.at[pl.ds((3 - p) * stride, cap), :], ours_rows.at[1 - p], load_sem.at[p])
        for p in range(2)
    ]
    weights = [
        remote(w1_ref, w1p_ref, w_send.at[0], w_recv.at[0], partner),
        remote(w2_ref, w2p_ref, w_send.at[1], w_recv.at[1], partner),
    ]
    for p in range(2):
        pair[p].start()
        loads[p].start()
    for copy in weights:
        copy.start()

    def fetch_weights(step, slot, start):
        @pl.when(step < w_steps)
        def _():
            cols = pl.ds(pl.multiple_of(step * WIDTH, WIDTH), WIDTH)
            start(pltpu.make_async_copy(w1_ref.at[:, cols], w1_buf.at[slot], w_sem.at[0, slot]))
            start(pltpu.make_async_copy(w2_ref.at[cols, :], w2_buf.at[slot], w_sem.at[1, slot]))

        @pl.when(step >= w_steps)
        def _():
            cols = pl.ds(pl.multiple_of((step - w_steps) * WIDTH, WIDTH), WIDTH)
            start(pltpu.make_async_copy(w1p_ref.at[:, cols], w1_buf.at[slot], w_sem.at[0, slot]))
            start(pltpu.make_async_copy(w2p_ref.at[cols, :], w2_buf.at[slot], w_sem.at[1, slot]))

    fetch_weights(0, 0, lambda copy: copy.start())

    cross = [
        remote(ours_rows.at[1 - p], inbox.at[p], x_send.at[p], x_recv.at[p], other) for p in range(2)
    ]
    for p in range(2):
        b = 1 - p
        loads[p].wait()
        pair[p].wait_recv()

        @pl.loop(0, cap // TILE)
        def _(t, p=p, b=b):
            span = pl.ds(pl.multiple_of(t * TILE, TILE), TILE)
            source = source_ref[b, span, :]
            mine = ours_rows[b, span, :].astype(jnp.float32)
            theirs = inbox[p, span, :].astype(jnp.float32)
            ours_rows[b, span, :] = jnp.where(
                source == 0, mine, jnp.where(source == 1, theirs, 0.0)
            ).astype(jnp.bfloat16)

        pl.semaphore_signal(ready.at[p], inc=1, device_id=(dp, other), device_id_type=MESH)
        pl.semaphore_wait(ready.at[p], 1)
        cross[p].start()

    gain = gain_ref[...].astype(jnp.float32)

    def send_sums(piece):
        span = pl.ds(pl.multiple_of(piece * PIECE, PIECE), PIECE)
        return remote(acc.at[span, :], sums_ref.at[span, :], s_send.at[piece], s_recv.at[piece], other)

    @pl.loop(0, 2)
    def _(b):
        remote(ours_rows.at[b], inbox.at[b], x_send.at[b], x_recv.at[b], other).wait_recv()

        @pl.loop(0, n_tok // 256)
        def _(t):
            span = pl.ds(pl.multiple_of(t * 256, 256), 256)
            slot = lax.broadcasted_iota(jnp.int32, (256, cap), 1)
            pick_ours = (slot == ours_ref[b, span, :]).astype(jnp.float32).astype(jnp.bfloat16)
            pick_other = (slot == other_ref[b, span, :]).astype(jnp.float32).astype(jnp.bfloat16)
            rows = jnp.dot(pick_ours, ours_rows[b], preferred_element_type=jnp.float32) + jnp.dot(
                pick_other, inbox[b], preferred_element_type=jnp.float32
            )
            kept[span, :] = rows.astype(jnp.bfloat16)
            inv_rms = lax.rsqrt(jnp.mean(rows * rows, axis=-1, keepdims=True) + RMS_EPS)
            normed[span, :] = (rows * inv_rms * gain).astype(jnp.bfloat16)

        @pl.loop(0, n_chunks)
        def _(chunk):
            tok = pl.ds(pl.multiple_of(chunk * CHUNK, CHUNK), CHUNK)
            out_rows = pl.ds(pl.multiple_of(b * n_tok + chunk * CHUNK, CHUNK), CHUNK)
            acc[out_rows, :] = jnp.zeros((CHUNK, dim), jnp.float32)

            @pl.loop(0, 2 * w_steps)
            def _(w):
                step = (b * n_chunks + chunk) * 2 * w_steps + w
                slot = lax.rem(step, 2)
                fetch_weights(w, slot, lambda copy: copy.wait())

                @pl.when(step == w_steps - 1)
                def _():
                    for copy in weights:
                        copy.wait_recv()

                @pl.when(step + 1 < 2 * n_chunks * 2 * w_steps)
                def _():
                    fetch_weights(lax.rem(step + 1, 2 * w_steps), 1 - slot, lambda copy: copy.start())

                parts = []
                for half in range(2):
                    cols = pl.ds(half * (WIDTH // 2), WIDTH // 2)
                    z = jnp.dot(normed[tok, :], w1_buf[slot, :, cols], preferred_element_type=jnp.float32)
                    z = z.astype(jnp.bfloat16).astype(jnp.float32)
                    inner = 0.7978845608028654 * (z + 0.044715 * (z * z * z))
                    parts.append((0.5 * z * (1.0 + jnp.tanh(inner))).astype(jnp.bfloat16))
                hidden = jnp.concatenate(parts, axis=1)
                for half in range(2):
                    cols = pl.ds(half * (dim // 2), dim // 2)
                    acc[out_rows, cols] += jnp.dot(
                        hidden, w2_buf[slot, :, cols], preferred_element_type=jnp.float32
                    )

            @pl.when(b == 0)
            def _():
                for q in range(CHUNK // PIECE):
                    send_sums(chunk * (CHUNK // PIECE) + q).start()

    def take_sums(piece, slot):
        span = pl.ds(pl.multiple_of(piece * PIECE, PIECE), PIECE)
        return pltpu.make_async_copy(sums_ref.at[span, :], sum_buf.at[slot], r_sem.at[slot])

    def put_out(piece, slot):
        span = pl.ds(pl.multiple_of(piece * PIECE, PIECE), PIECE)
        return pltpu.make_async_copy(out_buf.at[slot], out_ref.at[span, :], o_sem.at[slot])

    @pl.loop(0, n_pieces)
    def _(piece):
        slot = lax.rem(piece, 2)
        send_sums(piece).wait_recv()
        take = take_sums(piece, slot)
        take.start()
        take.wait()

        @pl.when(piece >= 2)
        def _():
            put_out(piece - 2, slot).wait()

        span = pl.ds(pl.multiple_of(piece * PIECE, PIECE), PIECE)
        own = pl.ds(pl.multiple_of(n_tok + piece * PIECE, PIECE), PIECE)
        total = acc[own, :] + sum_buf[slot]
        out_buf[slot] = (kept[span, :].astype(jnp.float32) + total).astype(jnp.bfloat16)
        put_out(piece, slot).start()

    put_out(n_pieces - 2, lax.rem(n_pieces - 2, 2)).wait()
    put_out(n_pieces - 1, lax.rem(n_pieces - 1, 2)).wait()

    for copy in pair + weights + cross:
        copy.wait_send()

    @pl.loop(0, n_pieces)
    def _(piece):
        send_sums(piece).wait_send()


def mlp_block(cap, collective_id, gain, from_ours, from_other, source, rows, w_in, w_out):
    n_tok = rows.shape[0] // 4
    dim, width = w_in.shape
    any_spec, vmem = pl.BlockSpec(memory_space=pl.ANY), pl.BlockSpec(memory_space=pltpu.VMEM)
    dma = pltpu.SemaphoreType.DMA
    n_pieces = n_tok // PIECE
    flops = 2 * (2 * n_tok) * dim * (2 * width) * 2
    return pl.pallas_call(
        functools.partial(block_kernel, cap, n_tok),
        out_shape=[
            jax.ShapeDtypeStruct((n_tok, dim), jnp.bfloat16),
            jax.ShapeDtypeStruct(w_in.shape, w_in.dtype),
            jax.ShapeDtypeStruct(w_out.shape, w_out.dtype),
            jax.ShapeDtypeStruct((n_tok, dim), jnp.float32),
        ],
        in_specs=[vmem, vmem, vmem, vmem, any_spec, any_spec, any_spec],
        out_specs=[any_spec] * 4,
        scratch_shapes=[
            pltpu.VMEM((2, cap, dim), jnp.bfloat16),
            pltpu.VMEM((2, cap, dim), jnp.bfloat16),
            pltpu.VMEM((n_tok, dim), jnp.bfloat16),
            pltpu.VMEM((n_tok, dim), jnp.bfloat16),
            pltpu.VMEM((2 * n_tok, dim), jnp.float32),
            pltpu.VMEM((2, dim, WIDTH), jnp.bfloat16),
            pltpu.VMEM((2, WIDTH, dim), jnp.bfloat16),
            pltpu.VMEM((2, PIECE, dim), jnp.float32),
            pltpu.VMEM((2, PIECE, dim), jnp.bfloat16),
            dma((2,)), dma((2,)), dma((2,)), dma((2,)), dma((2,)),
            pltpu.SemaphoreType.REGULAR((2,)),
            dma((2,)), dma((2,)), dma((2, 2)), dma((n_pieces,)), dma((n_pieces,)), dma((2,)), dma((2,)),
        ],
        compiler_params=pltpu.CompilerParams(
            collective_id=collective_id, has_side_effects=True, vmem_limit_bytes=67043328
        ),
        cost_estimate=pl.CostEstimate(flops=flops, bytes_accessed=1 << 28, transcendentals=0),
        name="mlp_block",
    )(gain, from_ours, from_other, source[:, :cap], rows, w_in, w_out)[0]


def solution(mesh):
    swap = [(0, 1), (1, 0)]

    def device_step(token_ids, table_shard, norm_gain, w_in_shard, w_out_shard):
        n_tok = token_ids.shape[0] // 4
        *lists, from_ours, from_other, source, most = prepare(token_ids, table_shard.shape[0], n_tok)
        most = jnp.full((8, 128), most, jnp.int32)
        most = jnp.max(jnp.maximum(most, lax.ppermute(most, "dp", swap)))
        rows = gather_rows(table_shard, *lists, n_tok)
        return lax.cond(
            most <= PACKED,
            functools.partial(mlp_block, PACKED, 0),
            functools.partial(mlp_block, n_tok, 1),
            norm_gain[None, :], from_ours, from_other, source, rows, w_in_shard, w_out_shard,
        )

    return jax.shard_map(
        device_step,
        mesh=mesh,
        in_specs=(P("dp"), P("tp", None), P(), P(None, "tp"), P("tp", None)),
        out_specs=P(("dp", "tp"), None),
        check_vma=False,
    )
```

```python
import functools

import jax
import jax.numpy as jnp
from jax import lax
from jax.experimental import pallas as pl
from jax.experimental.pallas import tpu as pltpu
from jax.sharding import PartitionSpec as P

RMS_EPS = 1e-6
TILE = 32
SLOTS = 6
PARTS = 4
PIECE = 128
CHUNK = 512
WIDTH = 512
PACKED = 704
MESH = pl.DeviceIdType.MESH


def ones_where(cond):
    return jnp.where(cond, 1.0, 0.0).astype(jnp.bfloat16)


def exact_dot(lhs, rhs):
    return jnp.dot(lhs.astype(jnp.bfloat16), rhs.astype(jnp.bfloat16), preferred_element_type=jnp.float32)


def gather_kernel(
    shard_rows, tokens_ref, table_ref, out_ref, place_ref, counts_ref,
    meta, meta_smem, picks, slabs, rows, steps, meta_sem, slab_sem, row_sem,
):
    me = lax.axis_index("tp")
    chip, core = lax.div(me, 2), lax.rem(me, 2)
    partner, other = me + 1 - 2 * core, lax.rem(me + 2, 4)
    other_partner = other + 1 - 2 * core
    blocks = [other_partner, partner, other, me]
    groups = meta.shape[0] // 3
    per = groups // 4

    ids = jnp.concatenate([tokens_ref[pl.ds(pl.multiple_of(b * per, per), per), :] for b in blocks], axis=0)
    owner = sum((ids >= q * shard_rows).astype(jnp.int32) for q in (1, 2, 3))
    mask = jnp.concatenate([jnp.where(owner == q, 1.0, 0.0) for q in range(4)], axis=0).astype(jnp.bfloat16)
    r = lax.broadcasted_iota(jnp.int32, (128, 128), 0)
    c = lax.broadcasted_iota(jnp.int32, (128, 128), 1)
    same = lax.div(r, per) == lax.div(c, per)
    ones = jnp.ones((128, 128), jnp.bfloat16)
    rank = exact_dot(mask, ones_where(r <= c)) + exact_dot(exact_dot(ones_where(same & (c < r)), mask), ones)
    total = exact_dot(exact_dot(ones_where(same), mask), ones)
    rank = [rank[q * groups:(q + 1) * groups] for q in range(4)]
    total = [total[q * groups:(q + 1) * groups] for q in range(4)]
    place = jnp.where(owner == 0, rank[0], jnp.where(
        owner == 1, rank[1] + total[0], jnp.where(owner == 2, rank[2], rank[3] + total[2])
    )).astype(jnp.int32) - 1
    ours = lax.shift_right_logical(owner, 1) == chip
    place_ref[0] = jnp.where(ours, place, -1)[groups // 2:].astype(jnp.float32)
    place_ref[1] = jnp.where(ours, -1, place)[groups // 2:].astype(jnp.float32)
    meta[pl.ds(groups, groups), :] = jnp.where(chip == 0, total[0], total[2]).astype(jnp.int32)
    meta[pl.ds(2 * groups, groups), :] = jnp.where(chip == 0, total[1], total[3]).astype(jnp.int32)

    local = jnp.where(owner == me, ids - me * shard_rows, 0)
    mine = owner == me
    high, low = lax.shift_right_logical(local, 8).astype(jnp.float32), (local & 255).astype(jnp.float32)
    place_group = lax.shift_right_logical(place, 7)
    eye = ones_where(r == c)
    dims = (((1,), (1,)), ((), ()))
    lane_of = lax.dot_general(
        eye, (place & 127).astype(jnp.float32).astype(jnp.bfloat16), dims, preferred_element_type=jnp.float32
    ).astype(jnp.int32)
    group_row = lax.broadcasted_iota(jnp.int32, (per, 128), 0)
    found = []
    for b in range(4):
        acc = jnp.zeros((2 * per, 128), jnp.float32)
        for g in range(b * per, (b + 1) * per):
            hit = (place_group[g:g + 1] == group_row) & mine[g:g + 1]
            lhs = jnp.concatenate([jnp.where(hit, high[g:g + 1], 0.0), jnp.where(hit, low[g:g + 1], 0.0)], axis=0)
            acc = acc + exact_dot(lhs, ones_where(lane_of[:, g:g + 1] == c))
        found.append(acc[:per] * 256.0 + acc[per:])
    found = jnp.concatenate(found, axis=0).astype(jnp.int32)
    meta[pl.ds(0, groups), :] = lax.shift_right_logical(found, 3)
    row_of = lax.dot_general(
        eye, (found & 7).astype(jnp.float32).astype(jnp.bfloat16), dims, preferred_element_type=jnp.float32
    ).astype(jnp.int32)
    for g in range(groups):
        picks[pl.ds(g * 128, 128), :] = jnp.broadcast_to(row_of[:, g:g + 1], (128, 128))

    to_smem = pltpu.make_async_copy(meta, meta_smem, meta_sem)
    to_smem.start()
    to_smem.wait()

    tiles = per * 128 // TILE
    n_steps = 0
    for b in range(4):
        count0, count1 = meta_smem[groups + b * per, 0], meta_smem[2 * groups + b * per, 0]
        if b >= 2:
            counts_ref[2 * (b - 2)] = count0
            counts_ref[2 * (b - 2) + 1] = count0 + count1
        start = jnp.where(core == 0, 0, count0)
        end = jnp.where(core == 0, count0, count0 + count1)
        first = lax.div(start, TILE)
        last = jnp.where(end > start, lax.div(end + TILE - 1, TILE), first)

        def note(t, _, b=b, first=first, n_steps=n_steps):
            steps[n_steps + t - first] = b * tiles + t
            return 0

        lax.fori_loop(first, last, note, 0)
        n_steps = n_steps + last - first

    def fetch(step):
        slot = lax.rem(step, SLOTS)
        tile = steps[step]
        group, lane = lax.div(tile, 128 // TILE), lax.rem(tile, 128 // TILE) * TILE
        for j in range(TILE):
            pltpu.make_async_copy(
                table_ref.at[meta_smem[group, lane + j]], slabs.at[slot, pl.ds(8 * j, 8), :], slab_sem.at[slot]
            ).start()

    for step in range(SLOTS - 1):
        @pl.when(step < n_steps)
        def _(step=step):
            fetch(step)

    def out_copy(step):
        slot = lax.rem(step, 2)
        return pltpu.make_async_copy(
            rows.at[slot], out_ref.at[pl.ds(steps[step] * TILE, TILE), :], row_sem.at[slot]
        )

    def work(step, _):
        @pl.when(step + SLOTS - 1 < n_steps)
        def _():
            fetch(step + SLOTS - 1)

        slot = lax.rem(step, SLOTS)
        pltpu.make_async_copy(slabs.at[slot], slabs.at[slot], slab_sem.at[slot]).wait()
        base = pl.multiple_of(steps[step] * TILE, TILE)
        pick = picks[pl.ds(base, TILE), :]
        col = lax.broadcasted_iota(jnp.int32, (TILE, 8 * TILE), 1)
        want = jnp.concatenate([pick] * (8 * TILE // 128), axis=1) + 8 * lax.broadcasted_iota(
            jnp.int32, (TILE, 8 * TILE), 0
        )

        @pl.when(step >= 2)
        def _():
            out_copy(step - 2).wait()

        rows[lax.rem(step, 2)] = exact_dot(ones_where(col == want), slabs[slot]).astype(jnp.bfloat16)
        out_copy(step).start()
        return 0

    lax.fori_loop(0, n_steps, work, 0)
    for back in (2, 1):
        @pl.when(n_steps >= back)
        def _(back=back):
            out_copy(n_steps - back).wait()


def gather_rows(token_ids, table_shard):
    n_ids, (shard_rows, dim) = token_ids.shape[0], table_shard.shape
    groups = n_ids // 128
    smem, vmem = pl.BlockSpec(memory_space=pltpu.SMEM), pl.BlockSpec(memory_space=pltpu.VMEM)
    return pl.pallas_call(
        functools.partial(gather_kernel, shard_rows),
        out_shape=[
            jax.ShapeDtypeStruct((n_ids, dim), jnp.bfloat16),
            jax.ShapeDtypeStruct((2, groups // 2, 128), jnp.float32),
            jax.ShapeDtypeStruct((4,), jnp.int32),
        ],
        in_specs=[vmem, pl.BlockSpec(memory_space=pl.ANY)],
        out_specs=[pl.BlockSpec(memory_space=pl.ANY), vmem, smem],
        scratch_shapes=[
            pltpu.VMEM((3 * groups, 128), jnp.int32),
            pltpu.SMEM((3 * groups, 128), jnp.int32),
            pltpu.VMEM((n_ids, 128), jnp.int32),
            pltpu.VMEM((SLOTS, 8 * TILE, dim), jnp.bfloat16),
            pltpu.VMEM((2, TILE, dim), jnp.bfloat16),
            pltpu.SMEM((n_ids // TILE,), jnp.int32),
            pltpu.SemaphoreType.DMA,
            pltpu.SemaphoreType.DMA((SLOTS,)),
            pltpu.SemaphoreType.DMA((2,)),
        ],
        compiler_params=pltpu.CompilerParams(vmem_limit_bytes=40 << 20),
        cost_estimate=pl.CostEstimate(flops=1 << 34, bytes_accessed=1 << 26, transcendentals=0),
        name="gather_rows",
    )(token_ids.reshape(groups, 128), table_shard.reshape(-1, 8, dim))


def block_kernel(
    cap, stride, gain_ref, place_ref, counts_ref, rows_ref, w1_ref, w2_ref,
    out_ref, w1p_ref, w2p_ref, sums_ref,
    inbox, ours_rows, normed, kept, acc, w1_buf, w2_buf, sum_buf, out_buf,
    pair_send, pair_recv, load_sem, w_send, w_recv, ready, x_send, x_recv, w_sem, s_send, s_recv, r_sem, o_sem,
):
    me, dp = lax.axis_index("tp"), lax.axis_index("dp")
    core = lax.rem(me, 2)
    partner = me + 1 - 2 * core
    other = lax.rem(me + 2, 4)
    dim = gain_ref.shape[1]
    n_tok = out_ref.shape[0]
    width = w1_ref.shape[1]
    w_steps = width // WIDTH
    n_chunks = n_tok // CHUNK
    n_pieces = n_tok // PIECE

    barrier = pltpu.get_barrier_semaphore()
    for peer in (partner, other):
        pl.semaphore_signal(barrier, inc=1, device_id=(dp, peer), device_id_type=MESH)
    pl.semaphore_wait(barrier, 2)

    def remote(src, dst, send, recv, peer):
        return pltpu.make_async_remote_copy(
            src_ref=src, dst_ref=dst, send_sem=send, recv_sem=recv, device_id=(dp, peer), device_id_type=MESH
        )

    part = cap // PARTS
    parts = [(p, q) for p in range(2) for q in range(PARTS)]

    def pair(p, q):
        src = pl.ds((1 - p) * stride + q * part, part)
        return remote(
            rows_ref.at[src, :], inbox.at[p, pl.ds(q * part, part), :], pair_send.at[p, q], pair_recv.at[p, q], partner
        )

    def load(p, q):
        src = pl.ds((3 - p) * stride + q * part, part)
        return pltpu.make_async_copy(
            rows_ref.at[src, :], ours_rows.at[1 - p, pl.ds(q * part, part), :], load_sem.at[p, q]
        )

    def cross(p, q):
        span = pl.ds(q * part, part)
        return remote(
            ours_rows.at[1 - p, span, :], inbox.at[p, span, :], x_send.at[p, q], x_recv.at[p, q], other
        )

    weights = [
        remote(w1_ref, w1p_ref, w_send.at[0], w_recv.at[0], partner),
        remote(w2_ref, w2p_ref, w_send.at[1], w_recv.at[1], partner),
    ]
    for p, q in parts:
        pair(p, q).start()
        load(p, q).start()
    for copy in weights:
        copy.start()

    def fetch_weights(step, slot, start):
        @pl.when(step < w_steps)
        def _():
            cols = pl.ds(pl.multiple_of(step * WIDTH, WIDTH), WIDTH)
            start(pltpu.make_async_copy(w1_ref.at[:, cols], w1_buf.at[slot], w_sem.at[0, slot]))
            start(pltpu.make_async_copy(w2_ref.at[cols, :], w2_buf.at[slot], w_sem.at[1, slot]))

        @pl.when(step >= w_steps)
        def _():
            cols = pl.ds(pl.multiple_of((step - w_steps) * WIDTH, WIDTH), WIDTH)
            start(pltpu.make_async_copy(w1p_ref.at[:, cols], w1_buf.at[slot], w_sem.at[0, slot]))
            start(pltpu.make_async_copy(w2p_ref.at[cols, :], w2_buf.at[slot], w_sem.at[1, slot]))

    fetch_weights(0, 0, lambda copy: copy.start())

    for p, q in parts:
        b = 1 - p
        load(p, q).wait()
        pair(p, q).wait_recv()
        core0_end, chip_end = counts_ref[2 * b], counts_ref[2 * b + 1]

        @pl.loop(0, part // 16)
        def _(t, p=p, q=q, b=b, core0_end=core0_end, chip_end=chip_end):
            base = pl.multiple_of(q * part + t * 16, 16)
            span = pl.ds(base, 16)
            pos = base + lax.broadcasted_iota(jnp.int32, (16, dim), 0)
            mine = ours_rows[b, span, :].astype(jnp.float32)
            theirs = inbox[p, span, :].astype(jnp.float32)
            from_core = jnp.where(pos < core0_end, 0, 1)
            merged = jnp.where(from_core == core, mine, theirs)
            ours_rows[b, span, :] = jnp.where(pos < chip_end, merged, 0.0).astype(jnp.bfloat16)

        pl.semaphore_signal(ready.at[p, q], inc=1, device_id=(dp, other), device_id_type=MESH)
        pl.semaphore_wait(ready.at[p, q], 1)
        cross(p, q).start()

    gain = gain_ref[...].astype(jnp.float32)

    sums_land = sum_buf if cap < n_tok else sums_ref

    def send_sums(piece):
        span = pl.ds(pl.multiple_of(piece * PIECE, PIECE), PIECE)
        return remote(acc.at[span, :], sums_land.at[span, :], s_send.at[piece], s_recv.at[piece], other)

    @pl.loop(0, 2)
    def _(b):
        for q in range(PARTS):
            span = pl.ds(q * part, part)
            remote(
                ours_rows.at[1 - b, span, :], inbox.at[b, span, :], x_send.at[b, q], x_recv.at[b, q], other
            ).wait_recv()

        @pl.loop(0, n_tok // 256)
        def _(t):
            span = pl.ds(pl.multiple_of(t * 256, 256), 256)
            slot = lax.broadcasted_iota(jnp.int32, (128, cap), 1).astype(jnp.float32)
            diagonal = lax.broadcasted_iota(jnp.int32, (128, 128), 0) == lax.broadcasted_iota(
                jnp.int32, (128, 128), 1
            )

            def pick_from(side):
                picks = []
                for g in range(2):
                    row = place_ref[side, pl.ds(b * (n_tok // 128) + 2 * t + g, 1), :]
                    column = jnp.sum(jnp.where(diagonal, row, 0.0), axis=1, keepdims=True)
                    picks.append(ones_where(slot == column))
                return jnp.concatenate(picks, axis=0)

            pick_ours, pick_other = pick_from(0), pick_from(1)
            rows = jnp.dot(pick_ours, ours_rows[b], preferred_element_type=jnp.float32) + jnp.dot(
                pick_other, inbox[b], preferred_element_type=jnp.float32
            )
            kept[span, :] = rows.astype(jnp.bfloat16)
            inv_rms = lax.rsqrt(jnp.mean(rows * rows, axis=-1, keepdims=True) + RMS_EPS)
            normed[span, :] = (rows * inv_rms * gain).astype(jnp.bfloat16)

        @pl.loop(0, n_chunks)
        def _(chunk):
            tok = pl.ds(pl.multiple_of(chunk * CHUNK, CHUNK), CHUNK)
            out_rows = pl.ds(pl.multiple_of(b * n_tok + chunk * CHUNK, CHUNK), CHUNK)
            acc[out_rows, :] = jnp.zeros((CHUNK, dim), jnp.float32)

            @pl.loop(0, 2 * w_steps)
            def _(w):
                step = (b * n_chunks + chunk) * 2 * w_steps + w
                slot = lax.rem(step, 2)
                fetch_weights(w, slot, lambda copy: copy.wait())

                @pl.when(step == w_steps - 1)
                def _():
                    for copy in weights:
                        copy.wait_recv()

                @pl.when(step + 1 < 2 * n_chunks * 2 * w_steps)
                def _():
                    fetch_weights(lax.rem(step + 1, 2 * w_steps), 1 - slot, lambda copy: copy.start())

                parts = []
                for half in range(2):
                    cols = pl.ds(half * (WIDTH // 2), WIDTH // 2)
                    z = jnp.dot(normed[tok, :], w1_buf[slot, :, cols], preferred_element_type=jnp.float32)
                    z = z.astype(jnp.bfloat16).astype(jnp.float32)
                    inner = 0.7978845608028654 * (z + 0.044715 * (z * z * z))
                    parts.append((0.5 * z * (1.0 + jnp.tanh(inner))).astype(jnp.bfloat16))
                hidden = jnp.concatenate(parts, axis=1)
                for half in range(2):
                    cols = pl.ds(half * (dim // 2), dim // 2)
                    acc[out_rows, cols] += jnp.dot(
                        hidden, w2_buf[slot, :, cols], preferred_element_type=jnp.float32
                    )

            @pl.when(b == 0)
            def _():
                for q in range(CHUNK // PIECE):
                    send_sums(chunk * (CHUNK // PIECE) + q).start()

    sums_in_vmem = cap < n_tok

    def take_sums(piece, slot):
        span = pl.ds(pl.multiple_of(piece * PIECE, PIECE), PIECE)
        return pltpu.make_async_copy(sums_ref.at[span, :], sum_buf.at[slot], r_sem.at[slot])

    def put_out(piece, slot):
        span = pl.ds(pl.multiple_of(piece * PIECE, PIECE), PIECE)
        return pltpu.make_async_copy(out_buf.at[slot], out_ref.at[span, :], o_sem.at[slot])

    @pl.loop(0, n_pieces)
    def _(piece):
        slot = lax.rem(piece, 2)
        send_sums(piece).wait_recv()
        if not sums_in_vmem:
            take = take_sums(piece, slot)
            take.start()
            take.wait()

        @pl.when(piece >= 2)
        def _():
            put_out(piece - 2, slot).wait()

        span = pl.ds(pl.multiple_of(piece * PIECE, PIECE), PIECE)
        own = pl.ds(pl.multiple_of(n_tok + piece * PIECE, PIECE), PIECE)
        total = acc[own, :] + (sums_land[span, :] if sums_in_vmem else sum_buf[slot])
        out_buf[slot] = (kept[span, :].astype(jnp.float32) + total).astype(jnp.bfloat16)
        put_out(piece, slot).start()

    put_out(n_pieces - 2, lax.rem(n_pieces - 2, 2)).wait()
    put_out(n_pieces - 1, lax.rem(n_pieces - 1, 2)).wait()

    for copy in [pair(*at) for at in parts] + weights + [cross(*at) for at in parts]:
        copy.wait_send()

    @pl.loop(0, n_pieces)
    def _(piece):
        send_sums(piece).wait_send()


def mlp_block(cap, collective_id, gain, place, counts, rows, w_in, w_out):
    n_tok = rows.shape[0] // 4
    dim, width = w_in.shape
    any_spec, vmem = pl.BlockSpec(memory_space=pl.ANY), pl.BlockSpec(memory_space=pltpu.VMEM)
    smem = pl.BlockSpec(memory_space=pltpu.SMEM)
    dma = pltpu.SemaphoreType.DMA
    n_pieces = n_tok // PIECE
    flops = 2 * (2 * n_tok) * dim * (2 * width) * 2
    return pl.pallas_call(
        functools.partial(block_kernel, cap, n_tok),
        out_shape=[
            jax.ShapeDtypeStruct((n_tok, dim), jnp.bfloat16),
            jax.ShapeDtypeStruct(w_in.shape, w_in.dtype),
            jax.ShapeDtypeStruct(w_out.shape, w_out.dtype),
            jax.ShapeDtypeStruct((n_tok if cap == n_tok else 8, dim), jnp.float32),
        ],
        in_specs=[vmem, vmem, smem, any_spec, any_spec, any_spec],
        out_specs=[any_spec] * 4,
        scratch_shapes=[
            pltpu.VMEM((2, cap, dim), jnp.bfloat16),
            pltpu.VMEM((2, cap, dim), jnp.bfloat16),
            pltpu.VMEM((n_tok, dim), jnp.bfloat16),
            pltpu.VMEM((n_tok, dim), jnp.bfloat16),
            pltpu.VMEM((2 * n_tok, dim), jnp.float32),
            pltpu.VMEM((2, dim, WIDTH), jnp.bfloat16),
            pltpu.VMEM((2, WIDTH, dim), jnp.bfloat16),
            pltpu.VMEM((2, PIECE, dim) if cap == n_tok else (n_tok, dim), jnp.float32),
            pltpu.VMEM((2, PIECE, dim), jnp.bfloat16),
            dma((2, PARTS)), dma((2, PARTS)), dma((2, PARTS)), dma((2,)), dma((2,)),
            pltpu.SemaphoreType.REGULAR((2, PARTS)),
            dma((2, PARTS)), dma((2, PARTS)), dma((2, 2)), dma((n_pieces,)), dma((n_pieces,)), dma((2,)), dma((2,)),
        ],
        compiler_params=pltpu.CompilerParams(
            collective_id=collective_id, has_side_effects=True, vmem_limit_bytes=67043328
        ),
        cost_estimate=pl.CostEstimate(flops=flops, bytes_accessed=1 << 28, transcendentals=0),
        name="mlp_block",
    )(gain, place, counts, rows, w_in, w_out)[0]


def copy_kernel(src_ref, dst_ref, buf, in_sem, out_sem):
    n = buf.shape[0]
    rows = buf.shape[1]
    ins = [pltpu.make_async_copy(src_ref.at[pl.ds(i * rows, rows), :], buf.at[i], in_sem.at[i]) for i in range(n)]
    outs = [pltpu.make_async_copy(buf.at[i], dst_ref.at[pl.ds(i * rows, rows), :], out_sem.at[i]) for i in range(n)]
    for copy in ins:
        copy.start()
    for i in range(n):
        ins[i].wait()
        outs[i].start()
    for copy in outs:
        copy.wait()


def copy_out(x):
    n = 8
    return pl.pallas_call(
        copy_kernel,
        out_shape=jax.ShapeDtypeStruct(x.shape, x.dtype),
        in_specs=[pl.BlockSpec(memory_space=pl.ANY)],
        out_specs=pl.BlockSpec(memory_space=pl.ANY),
        scratch_shapes=[
            pltpu.VMEM((n, x.shape[0] // n, x.shape[1]), x.dtype),
            pltpu.SemaphoreType.DMA((n,)),
            pltpu.SemaphoreType.DMA((n,)),
        ],
        compiler_params=pltpu.CompilerParams(vmem_limit_bytes=62 << 20),
        name="copy_out",
    )(x)


def solution(mesh):
    swap = [(0, 1), (1, 0)]

    def device_step(token_ids, table_shard, norm_gain, w_in_shard, w_out_shard):
        n_tok = token_ids.shape[0] // 4
        on_chip1 = jnp.sum((token_ids.reshape(4, n_tok) >= 2 * table_shard.shape[0]).astype(jnp.int32), axis=1)
        most = jnp.full((8, 128), jnp.max(jnp.maximum(on_chip1, n_tok - on_chip1)), jnp.int32)
        most = jnp.max(jnp.maximum(most, lax.ppermute(most, "dp", swap)))
        rows, place, counts = gather_rows(token_ids, table_shard)
        out = lax.cond(
            most <= PACKED,
            functools.partial(mlp_block, PACKED, 0),
            functools.partial(mlp_block, n_tok, 1),
            norm_gain[None, :], place, counts, rows, w_in_shard, w_out_shard,
        )
        return copy_out(out)

    return jax.shard_map(
        device_step,
        mesh=mesh,
        in_specs=(P("dp"), P("tp", None), P(), P(None, "tp"), P("tp", None)),
        out_specs=P(("dp", "tp"), None),
        check_vma=False,
    )
```

```python
import functools

import jax
import jax.numpy as jnp
from jax import lax
from jax.experimental import pallas as pl
from jax.experimental.pallas import tpu as pltpu
from jax.sharding import PartitionSpec as P

RMS_EPS = 1e-6
TILE = 64
PICK = 32
SLOTS = 4
EARLY = 128
GROUPS = 16
PIECE = 128
CHUNK = 512
WIDTH = 512
PACKED = (672, 704)
MESH = pl.DeviceIdType.MESH


def ones_where(cond):
    return jnp.where(cond, 1.0, 0.0).astype(jnp.bfloat16)


def exact_dot(lhs, rhs):
    return jnp.dot(lhs.astype(jnp.bfloat16), rhs.astype(jnp.bfloat16), preferred_element_type=jnp.float32)


def fetch_slabs(table_ref, slab_ids, group, lane, slabs, slot, sem):
    for j in range(TILE):
        pltpu.make_async_copy(
            table_ref.at[slab_ids(group, lane + j)], slabs.at[slot, pl.ds(8 * j, 8), :], sem.at[slot]
        ).start()


def pick_rows(picks, base, slabs, slot, sem, rows, row_slot):
    pltpu.make_async_copy(slabs.at[slot], slabs.at[slot], sem.at[slot]).wait()
    col = lax.broadcasted_iota(jnp.int32, (PICK, 8 * PICK), 1)
    first_col = 8 * lax.broadcasted_iota(jnp.int32, (PICK, 8 * PICK), 0)
    for part in range(TILE // PICK):
        pick = picks[pl.ds(base + part * PICK, PICK), :]
        want = jnp.concatenate([pick] * (8 * PICK // 128), axis=1) + first_col
        rows[row_slot, pl.ds(part * PICK, PICK), :] = exact_dot(
            ones_where(col == want), slabs[slot, pl.ds(part * 8 * PICK, 8 * PICK), :]
        ).astype(jnp.bfloat16)


def to_column(eye, values):
    return lax.dot_general(
        eye, values.astype(jnp.float32).astype(jnp.bfloat16), (((1,), (1,)), ((), ())),
        preferred_element_type=jnp.float32,
    ).astype(jnp.int32)


def early_kernel(
    shard_rows, tokens_ref, table_ref, part_ref, mine_ref, found_ref, place_ref, counts_ref, rests_ref,
    slab_no, slab_no_smem, picks, slabs, rows, meta_sem, slab_sem, row_sem,
):
    me = lax.axis_index("tp")
    chip, core = lax.div(me, 2), lax.rem(me, 2)
    partner, other = me + 1 - 2 * core, lax.rem(me + 2, 4)
    other_partner = other + 1 - 2 * core
    blocks = [other_partner, partner, other, me]
    groups = tokens_ref.shape[0]
    per = groups // 4

    ids = jnp.concatenate([tokens_ref[pl.ds(pl.multiple_of(b * per, per), per), :] for b in blocks], axis=0)
    owner = sum((ids >= q * shard_rows).astype(jnp.int32) for q in (1, 2, 3))
    mask = jnp.concatenate([jnp.where(owner == q, 1.0, 0.0) for q in range(4)], axis=0).astype(jnp.bfloat16)
    r = lax.broadcasted_iota(jnp.int32, (128, 128), 0)
    c = lax.broadcasted_iota(jnp.int32, (128, 128), 1)
    same = lax.div(r, per) == lax.div(c, per)
    ones = jnp.ones((128, 128), jnp.bfloat16)
    rank = exact_dot(mask, ones_where(r <= c)) + exact_dot(exact_dot(ones_where(same & (c < r)), mask), ones)
    total = exact_dot(exact_dot(ones_where(same), mask), ones)
    rank = [rank[q * groups:(q + 1) * groups] - 1.0 for q in range(4)]
    rest = [jnp.maximum(total[q * groups:(q + 1) * groups] - EARLY, 0.0) for q in range(4)]

    def placed(q):
        late = EARLY + (rest[q - 1] if q % 2 else 0.0)
        return rank[q] + jnp.where(rank[q] < EARLY, float(EARLY * (q % 2)), late)

    place = jnp.where(owner == 0, placed(0), jnp.where(
        owner == 1, placed(1), jnp.where(owner == 2, placed(2), placed(3))
    )).astype(jnp.int32)
    ours = lax.shift_right_logical(owner, 1) == chip
    place_ref[0] = jnp.where(ours, place, -1)[groups // 2:].astype(jnp.float32)
    place_ref[1] = jnp.where(ours, -1, place)[groups // 2:].astype(jnp.float32)
    counts_ref[pl.ds(0, groups), :] = jnp.where(chip == 0, rest[0], rest[2]).astype(jnp.int32)
    counts_ref[pl.ds(groups, groups), :] = jnp.where(chip == 0, rest[1], rest[3]).astype(jnp.int32)

    for i in range(4):
        row = (i % 2) * groups + (2 + i // 2) * per
        rests_ref[pl.ds(i, 1), :] = counts_ref[pl.ds(row, 1), :]

    mine = owner == me
    local = jnp.where(mine, ids - me * shard_rows, 0)
    high, low = lax.shift_right_logical(local, 8).astype(jnp.float32), (local & 255).astype(jnp.float32)
    place_group = lax.shift_right_logical(place, 7)
    eye = ones_where(r == c)
    lane_of = to_column(eye, place & 127)
    group_row = lax.broadcasted_iota(jnp.int32, (GROUPS, 128), 0)
    for b in (1, 3, 0, 2):
        acc = jnp.zeros((2 * GROUPS, 128), jnp.float32)
        for g in range(b * per, (b + 1) * per):
            hit = (place_group[g:g + 1] == group_row) & mine[g:g + 1]
            lhs = jnp.concatenate([jnp.where(hit, high[g:g + 1], 0.0), jnp.where(hit, low[g:g + 1], 0.0)], axis=0)
            acc = acc + exact_dot(lhs, ones_where(lane_of[:, g:g + 1] == c))
        found_ref[pl.ds(b * GROUPS, GROUPS), :] = (acc[:GROUPS] * 256.0 + acc[GROUPS:]).astype(jnp.int32)

    early_groups = 2 * EARLY // 128
    for i, b in enumerate((1, 3)):
        found = found_ref[pl.ds(b * GROUPS, GROUPS), :]
        slab_no[pl.ds(i * GROUPS, GROUPS), :] = lax.shift_right_logical(found, 3)
        row_of = to_column(eye, found & 7)
        for g in range(early_groups):
            picks[pl.ds((i * early_groups + g) * 128, 128), :] = jnp.broadcast_to(row_of[:, g:g + 1], (128, 128))
    to_smem = pltpu.make_async_copy(slab_no, slab_no_smem, meta_sem)
    to_smem.start()
    to_smem.wait()

    n = EARLY // TILE
    for i in range(2):
        for t in range(n):
            at = core * EARLY + t * TILE
            fetch_slabs(
                table_ref, lambda group, lane: slab_no_smem[group, lane],
                i * GROUPS + lax.div(at, 128), lax.rem(at, 128), slabs, i * n + t, slab_sem,
            )
    outs = []
    for i in range(2):
        for t in range(n):
            step = i * n + t
            base = pl.multiple_of(i * early_groups * 128 + core * EARLY + t * TILE, TILE)
            pick_rows(picks, base, slabs, step, slab_sem, rows, step)
            target = (part_ref, mine_ref)[i]
            outs.append(pltpu.make_async_copy(rows.at[step], target.at[pl.ds(t * TILE, TILE), :], row_sem.at[step]))
            outs[-1].start()
    for copy in outs:
        copy.wait()


def early_rows(token_ids, table):
    n_ids, (slab_count, _, dim) = token_ids.shape[0], table.shape
    groups, steps = n_ids // 128, 2 * EARLY // TILE
    any_spec, vmem = pl.BlockSpec(memory_space=pl.ANY), pl.BlockSpec(memory_space=pltpu.VMEM)
    rows = jax.ShapeDtypeStruct((EARLY, dim), jnp.bfloat16)
    return pl.pallas_call(
        functools.partial(early_kernel, 8 * slab_count),
        out_shape=[
            rows, rows,
            jax.ShapeDtypeStruct((4 * GROUPS, 128), jnp.int32),
            jax.ShapeDtypeStruct((2, groups // 2, 128), jnp.float32),
            jax.ShapeDtypeStruct((2 * groups, 128), jnp.int32),
            jax.ShapeDtypeStruct((4, 128), jnp.int32),
        ],
        in_specs=[vmem, any_spec],
        out_specs=[any_spec, any_spec, vmem, vmem, vmem, vmem],
        scratch_shapes=[
            pltpu.VMEM((2 * GROUPS, 128), jnp.int32),
            pltpu.SMEM((2 * GROUPS, 128), jnp.int32),
            pltpu.VMEM((4 * EARLY, 128), jnp.int32),
            pltpu.VMEM((steps, 8 * TILE, dim), jnp.bfloat16),
            pltpu.VMEM((steps, TILE, dim), jnp.bfloat16),
            pltpu.SemaphoreType.DMA,
            pltpu.SemaphoreType.DMA((steps,)),
            pltpu.SemaphoreType.DMA((steps,)),
        ],
        compiler_params=pltpu.CompilerParams(vmem_limit_bytes=40 << 20),
        cost_estimate=pl.CostEstimate(flops=1 << 32, bytes_accessed=1 << 25, transcendentals=0),
        name="early_rows",
    )(token_ids.reshape(groups, 128), table)


def gather_kernel(found_ref, counts_ref, found_vmem, table_ref, out_ref, picks, slabs, rows, steps, slab_sem, row_sem):
    core = lax.rem(lax.axis_index("tp"), 2)
    half = counts_ref.shape[0] // 2
    eye = ones_where(
        lax.broadcasted_iota(jnp.int32, (128, 128), 0) == lax.broadcasted_iota(jnp.int32, (128, 128), 1)
    )
    row_of = to_column(eye, found_vmem[...] & 7)
    per_block = out_ref.shape[0] // 4
    for b in range(4):
        for g in range(per_block // 128):
            picks[pl.ds(b * per_block + g * 128, 128), :] = jnp.broadcast_to(
                row_of[:, b * GROUPS + g:b * GROUPS + g + 1], (128, 128)
            )

    tiles = per_block // TILE
    n_steps = 0
    for b in (1, 3, 0, 2):
        rest0, rest1 = counts_ref[b * (half // 4), 0], counts_ref[half + b * (half // 4), 0]
        start = jnp.where(core == 0, 2 * EARLY, 2 * EARLY + rest0)
        end = jnp.where(core == 0, 2 * EARLY + rest0, 2 * EARLY + rest0 + rest1)
        if b % 2 == 0:
            for t in range(EARLY // TILE):
                steps[n_steps + t] = b * tiles + core * (EARLY // TILE) + t
            n_steps = n_steps + EARLY // TILE
        first = lax.div(start, TILE)
        last = jnp.where(end > start, lax.div(end + TILE - 1, TILE), first)

        def note(t, _, b=b, first=first, n_steps=n_steps):
            steps[n_steps + t - first] = b * tiles + t
            return 0

        lax.fori_loop(first, last, note, 0)
        n_steps = n_steps + last - first

    def fetch(step):
        tile = steps[step]
        at = lax.rem(tile, tiles) * TILE
        group = lax.div(tile, tiles) * GROUPS + lax.div(at, 128)
        fetch_slabs(
            table_ref, lambda g, lane: lax.shift_right_logical(found_ref[g, lane], 3),
            group, lax.rem(at, 128), slabs, lax.rem(step, SLOTS), slab_sem,
        )

    def first_fetch(step, _):
        fetch(step)
        return 0

    lax.fori_loop(0, jnp.minimum(n_steps, SLOTS - 1), first_fetch, 0)

    def out_copy(step):
        slot = lax.rem(step, 2)
        return pltpu.make_async_copy(
            rows.at[slot], out_ref.at[pl.ds(steps[step] * TILE, TILE), :], row_sem.at[slot]
        )

    def work(step, _):
        @pl.when(step + SLOTS - 1 < n_steps)
        def _():
            fetch(step + SLOTS - 1)

        @pl.when(step >= 2)
        def _():
            out_copy(step - 2).wait()

        base = pl.multiple_of(steps[step] * TILE, TILE)
        pick_rows(picks, base, slabs, lax.rem(step, SLOTS), slab_sem, rows, lax.rem(step, 2))
        out_copy(step).start()
        return 0

    lax.fori_loop(0, n_steps, work, 0)
    for back in (2, 1):
        @pl.when(n_steps >= back)
        def _(back=back):
            out_copy(n_steps - back).wait()


def gather_rows(found, counts, table, per_block):
    dim = table.shape[2]
    smem, vmem = pl.BlockSpec(memory_space=pltpu.SMEM), pl.BlockSpec(memory_space=pltpu.VMEM)
    return pl.pallas_call(
        gather_kernel,
        out_shape=jax.ShapeDtypeStruct((4 * per_block, dim), jnp.bfloat16),
        in_specs=[smem, smem, vmem, pl.BlockSpec(memory_space=pl.ANY)],
        out_specs=pl.BlockSpec(memory_space=pl.ANY),
        scratch_shapes=[
            pltpu.VMEM((4 * per_block, 128), jnp.int32),
            pltpu.VMEM((SLOTS, 8 * TILE, dim), jnp.bfloat16),
            pltpu.VMEM((2, TILE, dim), jnp.bfloat16),
            pltpu.SMEM((4 * per_block // TILE,), jnp.int32),
            pltpu.SemaphoreType.DMA((SLOTS,)),
            pltpu.SemaphoreType.DMA((2,)),
        ],
        compiler_params=pltpu.CompilerParams(vmem_limit_bytes=40 << 20),
        cost_estimate=pl.CostEstimate(flops=1 << 34, bytes_accessed=1 << 26, transcendentals=0),
        name="gather_rows",
    )(found, counts, found, table)


def block_kernel(
    cap, stride, parts, gain_ref, place_ref, counts_ref, part_ref, mine_ref, near_ref, far_ref, rows_ref, w1_ref, w2_ref,
    out_ref, w1p_ref, w2p_ref, sums_ref,
    inbox, ours_rows, normed, kept, acc, w1_buf, w2_buf, sum_buf, out_buf,
    pair_send, pair_recv, load_sem, w_send, w_recv, ready, x_send, x_recv, w_sem, s_send, s_recv, r_sem, o_sem, early_sem,
):
    me, dp = lax.axis_index("tp"), lax.axis_index("dp")
    core = lax.rem(me, 2)
    partner = me + 1 - 2 * core
    other = lax.rem(me + 2, 4)
    dim = gain_ref.shape[1]
    n_tok = out_ref.shape[0]
    width = w1_ref.shape[1]
    w_steps = width // WIDTH
    n_chunks = n_tok // CHUNK
    n_pieces = n_tok // PIECE

    barrier = pltpu.get_barrier_semaphore()
    for peer in (partner, other):
        pl.semaphore_signal(barrier, inc=1, device_id=(dp, peer), device_id_type=MESH)
    pl.semaphore_wait(barrier, 2)

    def remote(src, dst, send, recv, peer):
        return pltpu.make_async_remote_copy(
            src_ref=src, dst_ref=dst, send_sem=send, recv_sem=recv, device_id=(dp, peer), device_id_type=MESH
        )

    own_zone = pl.ds(pl.multiple_of(core * EARLY, EARLY), EARLY)
    partner_zone = pl.ds(pl.multiple_of((1 - core) * EARLY, EARLY), EARLY)

    def pair(i, p, at, n):
        src = pl.ds((1 - p) * stride + at, n)
        return remote(rows_ref.at[src, :], inbox.at[p, pl.ds(at, n), :], pair_send.at[i], pair_recv.at[i], partner)

    def load(i, p, at, n):
        src = pl.ds((3 - p) * stride + at, n)
        return pltpu.make_async_copy(rows_ref.at[src, :], ours_rows.at[1 - p, pl.ds(at, n), :], load_sem.at[i])

    def cross(i, p, at, n):
        span = pl.ds(at, n)
        return remote(ours_rows.at[1 - p, span, :], inbox.at[p, span, :], x_send.at[i], x_recv.at[i], other)

    pair_early = remote(part_ref, inbox.at[0, own_zone, :], early_sem.at[0], early_sem.at[1], partner)
    load_early = pltpu.make_async_copy(mine_ref, ours_rows.at[1, own_zone, :], early_sem.at[2])
    take_early = [
        pltpu.make_async_copy(near_ref, inbox.at[0, own_zone, :], early_sem.at[3]),
        pltpu.make_async_copy(far_ref, inbox.at[0, partner_zone, :], early_sem.at[4]),
    ]

    weights = [
        remote(w1_ref, w1p_ref, w_send.at[0], w_recv.at[0], partner),
        remote(w2_ref, w2p_ref, w_send.at[1], w_recv.at[1], partner),
    ]
    for i, part in enumerate(parts):
        pair(i, *part).start()
        load(i, *part).start()
    pair_early.start()
    load_early.start()
    for copy in weights:
        copy.start()

    def fetch_weights(step, slot, start):
        @pl.when(step < w_steps)
        def _():
            cols = pl.ds(pl.multiple_of(step * WIDTH, WIDTH), WIDTH)
            start(pltpu.make_async_copy(w1_ref.at[:, cols], w1_buf.at[slot], w_sem.at[0, slot]))
            start(pltpu.make_async_copy(w2_ref.at[cols, :], w2_buf.at[slot], w_sem.at[1, slot]))

        @pl.when(step >= w_steps)
        def _():
            cols = pl.ds(pl.multiple_of((step - w_steps) * WIDTH, WIDTH), WIDTH)
            start(pltpu.make_async_copy(w1p_ref.at[:, cols], w1_buf.at[slot], w_sem.at[0, slot]))
            start(pltpu.make_async_copy(w2p_ref.at[cols, :], w2_buf.at[slot], w_sem.at[1, slot]))

    fetch_weights(0, 0, lambda copy: copy.start())

    def merge(p, at, n):
        b = 1 - p
        core0_end = 2 * EARLY + counts_ref[2 * b, 0]
        chip_end = core0_end + counts_ref[2 * b + 1, 0]

        @pl.loop(0, n // 16)
        def _(t):
            base = pl.multiple_of(at + t * 16, 16)
            span = pl.ds(base, 16)
            pos = base + lax.broadcasted_iota(jnp.int32, (16, dim), 0)
            mine = ours_rows[b, span, :].astype(jnp.float32)
            theirs = inbox[p, span, :].astype(jnp.float32)
            if at >= 2 * EARLY:
                from_core0 = pos < core0_end
            else:
                from_core0 = (pos < EARLY) | ((pos >= 2 * EARLY) & (pos < core0_end))
            merged = jnp.where(jnp.where(from_core0, 0, 1) == core, mine, theirs)
            ours_rows[b, span, :] = jnp.where(pos < chip_end, merged, 0.0).astype(jnp.bfloat16)

    for i, part in enumerate(parts):
        load(i, *part).wait()
        pair(i, *part).wait_recv()
        merge(*part)
        pl.semaphore_signal(ready.at[i], inc=1, device_id=(dp, other), device_id_type=MESH)
        pl.semaphore_wait(ready.at[i], 1)
        cross(i, *part).start()
    load_early.wait()
    pair_early.wait_recv()
    merge(0, 0, 2 * EARLY)
    for copy in take_early:
        copy.start()
    for copy in take_early:
        copy.wait()

    gain = gain_ref[...].astype(jnp.float32)

    sums_land = sum_buf if cap < stride else sums_ref

    def send_sums(piece):
        span = pl.ds(pl.multiple_of(piece * PIECE, PIECE), PIECE)
        return remote(acc.at[span, :], sums_land.at[span, :], s_send.at[piece], s_recv.at[piece], other)

    @pl.loop(0, 2)
    def _(b):
        for p in range(2):
            @pl.when(b == p)
            def _(p=p):
                for i, part in enumerate(parts):
                    if part[0] == p:
                        cross(i, *part).wait_recv()

        @pl.loop(0, n_tok // 256)
        def _(t):
            span = pl.ds(pl.multiple_of(t * 256, 256), 256)
            slot = lax.broadcasted_iota(jnp.int32, (128, cap), 1).astype(jnp.float32)
            diagonal = lax.broadcasted_iota(jnp.int32, (128, 128), 0) == lax.broadcasted_iota(
                jnp.int32, (128, 128), 1
            )

            def pick_from(side):
                picks = []
                for g in range(2):
                    row = place_ref[side, pl.ds(b * (n_tok // 128) + 2 * t + g, 1), :]
                    column = jnp.sum(jnp.where(diagonal, row, 0.0), axis=1, keepdims=True)
                    picks.append(ones_where(slot == column))
                return jnp.concatenate(picks, axis=0)

            pick_ours, pick_other = pick_from(0), pick_from(1)
            rows = jnp.dot(pick_ours, ours_rows[b], preferred_element_type=jnp.float32) + jnp.dot(
                pick_other, inbox[b], preferred_element_type=jnp.float32
            )
            kept[span, :] = rows.astype(jnp.bfloat16)
            inv_rms = lax.rsqrt(jnp.mean(rows * rows, axis=-1, keepdims=True) + RMS_EPS)
            normed[span, :] = (rows * inv_rms * gain).astype(jnp.bfloat16)

        @pl.loop(0, n_chunks)
        def _(chunk):
            tok = pl.ds(pl.multiple_of(chunk * CHUNK, CHUNK), CHUNK)
            out_rows = pl.ds(pl.multiple_of(b * n_tok + chunk * CHUNK, CHUNK), CHUNK)
            acc[out_rows, :] = jnp.zeros((CHUNK, dim), jnp.float32)

            @pl.loop(0, 2 * w_steps)
            def _(w):
                step = (b * n_chunks + chunk) * 2 * w_steps + w
                slot = lax.rem(step, 2)
                fetch_weights(w, slot, lambda copy: copy.wait())

                @pl.when(step == w_steps - 1)
                def _():
                    for copy in weights:
                        copy.wait_recv()

                @pl.when(step + 1 < 2 * n_chunks * 2 * w_steps)
                def _():
                    fetch_weights(lax.rem(step + 1, 2 * w_steps), 1 - slot, lambda copy: copy.start())

                parts = []
                for half in range(2):
                    cols = pl.ds(half * (WIDTH // 2), WIDTH // 2)
                    z = jnp.dot(normed[tok, :], w1_buf[slot, :, cols], preferred_element_type=jnp.float32)
                    z = z.astype(jnp.bfloat16).astype(jnp.float32)
                    inner = 0.7978845608028654 * (z + 0.044715 * (z * z * z))
                    parts.append((0.5 * z * (1.0 + jnp.tanh(inner))).astype(jnp.bfloat16))
                hidden = jnp.concatenate(parts, axis=1)
                for half in range(2):
                    cols = pl.ds(half * (dim // 2), dim // 2)
                    acc[out_rows, cols] += jnp.dot(
                        hidden, w2_buf[slot, :, cols], preferred_element_type=jnp.float32
                    )

            @pl.when(b == 0)
            def _():
                for q in range(CHUNK // PIECE):
                    send_sums(chunk * (CHUNK // PIECE) + q).start()

    sums_in_vmem = cap < stride

    def take_sums(piece, slot):
        span = pl.ds(pl.multiple_of(piece * PIECE, PIECE), PIECE)
        return pltpu.make_async_copy(sums_ref.at[span, :], sum_buf.at[slot], r_sem.at[slot])

    def put_out(piece, slot):
        span = pl.ds(pl.multiple_of(piece * PIECE, PIECE), PIECE)
        return pltpu.make_async_copy(out_buf.at[slot], out_ref.at[span, :], o_sem.at[slot])

    @pl.loop(0, n_pieces)
    def _(piece):
        slot = lax.rem(piece, 2)
        send_sums(piece).wait_recv()
        if not sums_in_vmem:
            take = take_sums(piece, slot)
            take.start()
            take.wait()

        @pl.when(piece >= 2)
        def _():
            put_out(piece - 2, slot).wait()

        span = pl.ds(pl.multiple_of(piece * PIECE, PIECE), PIECE)
        own = pl.ds(pl.multiple_of(n_tok + piece * PIECE, PIECE), PIECE)
        total = acc[own, :] + (sums_land[span, :] if sums_in_vmem else sum_buf[slot])
        out_buf[slot] = (kept[span, :].astype(jnp.float32) + total).astype(jnp.bfloat16)
        put_out(piece, slot).start()

    put_out(n_pieces - 2, lax.rem(n_pieces - 2, 2)).wait()
    put_out(n_pieces - 1, lax.rem(n_pieces - 1, 2)).wait()

    sent = [pair(i, *part) for i, part in enumerate(parts)] + [cross(i, *part) for i, part in enumerate(parts)]
    for copy in [pair_early] + sent + weights:
        copy.wait_send()

    @pl.loop(0, n_pieces)
    def _(piece):
        send_sums(piece).wait_send()


def split_rows(p, first, last, ways=4):
    cuts = [first + 16 * ((last - first) // 16 * i // ways) for i in range(ways + 1)]
    return [(p, cuts[i], cuts[i + 1] - cuts[i]) for i in range(ways)]


def mlp_block(packed, collective_id, gain, place, counts, part, mine, near, far, rows, w_in, w_out):
    n_tok = place.shape[1] * 64
    stride = rows.shape[0] // 4
    cap = packed or stride
    parts = split_rows(0, 2 * EARLY, cap) + split_rows(1, 0, cap)
    n_parts = len(parts)
    dim, width = w_in.shape
    any_spec, vmem = pl.BlockSpec(memory_space=pl.ANY), pl.BlockSpec(memory_space=pltpu.VMEM)
    smem = pl.BlockSpec(memory_space=pltpu.SMEM)
    dma = pltpu.SemaphoreType.DMA
    n_pieces = n_tok // PIECE
    flops = 2 * (2 * n_tok) * dim * (2 * width) * 2
    return pl.pallas_call(
        functools.partial(block_kernel, cap, stride, parts),
        out_shape=[
            jax.ShapeDtypeStruct((n_tok, dim), jnp.bfloat16),
            jax.ShapeDtypeStruct(w_in.shape, w_in.dtype),
            jax.ShapeDtypeStruct(w_out.shape, w_out.dtype),
            jax.ShapeDtypeStruct((8 if packed else n_tok, dim), jnp.float32),
        ],
        in_specs=[vmem, vmem, smem] + [any_spec] * 7,
        out_specs=[any_spec] * 4,
        scratch_shapes=[
            pltpu.VMEM((2, cap, dim), jnp.bfloat16),
            pltpu.VMEM((2, cap, dim), jnp.bfloat16),
            pltpu.VMEM((n_tok, dim), jnp.bfloat16),
            pltpu.VMEM((n_tok, dim), jnp.bfloat16),
            pltpu.VMEM((2 * n_tok, dim), jnp.float32),
            pltpu.VMEM((2, dim, WIDTH), jnp.bfloat16),
            pltpu.VMEM((2, WIDTH, dim), jnp.bfloat16),
            pltpu.VMEM((n_tok, dim) if packed else (2, PIECE, dim), jnp.float32),
            pltpu.VMEM((2, PIECE, dim), jnp.bfloat16),
            dma((n_parts,)), dma((n_parts,)), dma((n_parts,)), dma((2,)), dma((2,)),
            pltpu.SemaphoreType.REGULAR((n_parts,)),
            dma((n_parts,)), dma((n_parts,)), dma((2, 2)), dma((n_pieces,)), dma((n_pieces,)), dma((2,)), dma((2,)), dma((5,)),
        ],
        compiler_params=pltpu.CompilerParams(
            collective_id=collective_id, has_side_effects=True, vmem_limit_bytes=67043328
        ),
        cost_estimate=pl.CostEstimate(flops=flops, bytes_accessed=1 << 28, transcendentals=0),
        name="mlp_block",
    )(gain, place, counts, part, mine, near, far, rows, w_in, w_out)[0]


def copy_kernel(src_ref, dst_ref, buf, in_sem, out_sem):
    n = buf.shape[0]
    rows = buf.shape[1]
    ins = [pltpu.make_async_copy(src_ref.at[pl.ds(i * rows, rows), :], buf.at[i], in_sem.at[i]) for i in range(n)]
    outs = [pltpu.make_async_copy(buf.at[i], dst_ref.at[pl.ds(i * rows, rows), :], out_sem.at[i]) for i in range(n)]
    for copy in ins:
        copy.start()
    for i in range(n):
        ins[i].wait()
        outs[i].start()
    for copy in outs:
        copy.wait()


def copy_out(x):
    n = 8
    return pl.pallas_call(
        copy_kernel,
        out_shape=jax.ShapeDtypeStruct(x.shape, x.dtype),
        in_specs=[pl.BlockSpec(memory_space=pl.ANY)],
        out_specs=pl.BlockSpec(memory_space=pl.ANY),
        scratch_shapes=[
            pltpu.VMEM((n, x.shape[0] // n, x.shape[1]), x.dtype),
            pltpu.SemaphoreType.DMA((n,)),
            pltpu.SemaphoreType.DMA((n,)),
        ],
        compiler_params=pltpu.CompilerParams(vmem_limit_bytes=62 << 20),
        name="copy_out",
    )(x)


def solution(mesh):
    swap = [(0, 1), (1, 0)]
    near_pairs = [(r, r ^ 2) for r in range(4)]
    far_pairs = [(r, r ^ 3) for r in range(4)]

    def device_step(token_ids, table_shard, norm_gain, w_in_shard, w_out_shard):
        shard_rows, dim = table_shard.shape
        n_tok = token_ids.shape[0] // 4
        by_block = token_ids.reshape(4, n_tok)
        above = [n_tok] + [jnp.sum((by_block >= q * shard_rows).astype(jnp.int32), axis=1) for q in (1, 2, 3)] + [0]
        rest = [jnp.maximum(above[q] - above[q + 1] - EARLY, 0) for q in range(4)]
        need = 2 * EARLY + jnp.max(jnp.maximum(rest[0] + rest[1], rest[2] + rest[3])).reshape(1)
        need = jnp.maximum(need, lax.ppermute(need, "dp", swap))[0]

        table = table_shard.reshape(-1, 8, dim)
        part, mine, found, place, counts, rests = early_rows(token_ids, table)
        near = lax.ppermute(mine, "tp", near_pairs)
        far = lax.ppermute(part, "tp", far_pairs)
        rows = gather_rows(found, counts, table, -(-(n_tok + EARLY) // 128) * 128)
        out = lax.switch(
            sum((need > cap).astype(jnp.int32) for cap in PACKED),
            [functools.partial(mlp_block, cap, i) for i, cap in enumerate(PACKED + (None,))],
            norm_gain[None, :], place, rests, part, mine, near, far, rows, w_in_shard, w_out_shard,
        )
        return copy_out(out)

    return jax.shard_map(
        device_step,
        mesh=mesh,
        in_specs=(P("dp"), P("tp", None), P(), P(None, "tp"), P("tp", None)),
        out_specs=P(("dp", "tp"), None),
        check_vma=False,
    )
```

```python
import functools

import jax
import jax.numpy as jnp
from jax import lax
from jax.experimental import pallas as pl
from jax.experimental.pallas import tpu as pltpu
from jax.sharding import PartitionSpec as P

RMS_EPS = 1e-6
TILE = 64
PICK = 32
SLOTS = 4
EARLY = 192
GROUPS = 16
PIECE = 128
CHUNK = 512
WIDTH = 512
PACKED = (672, 704)
MESH = pl.DeviceIdType.MESH


def ones_where(cond):
    return jnp.where(cond, 1.0, 0.0).astype(jnp.bfloat16)


def exact_dot(lhs, rhs):
    return jnp.dot(lhs.astype(jnp.bfloat16), rhs.astype(jnp.bfloat16), preferred_element_type=jnp.float32)


def fetch_slabs(table_ref, slab_ids, group, lane, slabs, slot, sem):
    for j in range(TILE):
        pltpu.make_async_copy(
            table_ref.at[slab_ids(group, lane + j)], slabs.at[slot, pl.ds(8 * j, 8), :], sem.at[slot]
        ).start()


def pick_rows(picks, base, slabs, slot, sem, rows, row_slot):
    pltpu.make_async_copy(slabs.at[slot], slabs.at[slot], sem.at[slot]).wait()
    col = lax.broadcasted_iota(jnp.int32, (PICK, 8 * PICK), 1)
    first_col = 8 * lax.broadcasted_iota(jnp.int32, (PICK, 8 * PICK), 0)
    for part in range(TILE // PICK):
        pick = picks[pl.ds(base + part * PICK, PICK), :]
        want = jnp.concatenate([pick] * (8 * PICK // 128), axis=1) + first_col
        rows[row_slot, pl.ds(part * PICK, PICK), :] = exact_dot(
            ones_where(col == want), slabs[slot, pl.ds(part * 8 * PICK, 8 * PICK), :]
        ).astype(jnp.bfloat16)


def to_column(eye, values):
    return lax.dot_general(
        eye, values.astype(jnp.float32).astype(jnp.bfloat16), (((1,), (1,)), ((), ())),
        preferred_element_type=jnp.float32,
    ).astype(jnp.int32)


def early_kernel(
    shard_rows, tokens_ref, table_ref, part_ref, mine_ref, found_ref, place_ref, counts_ref, need_ref,
    slab_no, slab_no_smem, picks, slabs, rows, meta_sem, slab_sem, row_sem,
):
    me = lax.axis_index("tp")
    chip, core = lax.div(me, 2), lax.rem(me, 2)
    partner, other = me + 1 - 2 * core, lax.rem(me + 2, 4)
    other_partner = other + 1 - 2 * core
    blocks = [other_partner, partner, other, me]
    groups = tokens_ref.shape[0]
    per = groups // 4

    ids = jnp.concatenate([tokens_ref[pl.ds(pl.multiple_of(b * per, per), per), :] for b in blocks], axis=0)
    owner = sum((ids >= q * shard_rows).astype(jnp.int32) for q in (1, 2, 3))
    mask = jnp.concatenate([jnp.where(owner == q, 1.0, 0.0) for q in range(4)], axis=0).astype(jnp.bfloat16)
    r = lax.broadcasted_iota(jnp.int32, (128, 128), 0)
    c = lax.broadcasted_iota(jnp.int32, (128, 128), 1)
    same = lax.div(r, per) == lax.div(c, per)
    ones = jnp.ones((128, 128), jnp.bfloat16)
    rank = exact_dot(mask, ones_where(r <= c)) + exact_dot(exact_dot(ones_where(same & (c < r)), mask), ones)
    total = exact_dot(exact_dot(ones_where(same), mask), ones)
    rank = [rank[q * groups:(q + 1) * groups] - 1.0 for q in range(4)]
    rest = [jnp.maximum(total[q * groups:(q + 1) * groups] - EARLY, 0.0) for q in range(4)]

    def placed(q):
        late = EARLY + (rest[q - 1] if q % 2 else 0.0)
        return rank[q] + jnp.where(rank[q] < EARLY, float(EARLY * (q % 2)), late)

    place = jnp.where(owner == 0, placed(0), jnp.where(
        owner == 1, placed(1), jnp.where(owner == 2, placed(2), placed(3))
    )).astype(jnp.int32)
    ours = lax.shift_right_logical(owner, 1) == chip
    place_ref[0] = jnp.where(ours, place, -1)[groups // 2:].astype(jnp.float32)
    place_ref[1] = jnp.where(ours, -1, place)[groups // 2:].astype(jnp.float32)
    for i, rests in enumerate((jnp.where(chip == 0, rest[0], rest[2]), jnp.where(chip == 0, rest[1], rest[3]))):
        for b in range(4):
            counts_ref[pl.ds(4 * i + b, 1), :] = rests[b * per:b * per + 1].astype(jnp.int32)
    need = jnp.max(jnp.maximum(rest[0] + rest[1], rest[2] + rest[3]), axis=0, keepdims=True)
    need_ref[...] = need.astype(jnp.int32) + 2 * EARLY

    mine = owner == me
    local = jnp.where(mine, ids - me * shard_rows, 0)
    high, low = lax.shift_right_logical(local, 8).astype(jnp.float32), (local & 255).astype(jnp.float32)
    place_group = lax.shift_right_logical(place, 7)
    eye = ones_where(r == c)
    lane_of = to_column(eye, place & 127)
    group_row = lax.broadcasted_iota(jnp.int32, (GROUPS, 128), 0)

    def find(b):
        acc = jnp.zeros((2 * GROUPS, 128), jnp.float32)
        for g in range(b * per, (b + 1) * per):
            hit = (place_group[g:g + 1] == group_row) & mine[g:g + 1]
            lhs = jnp.concatenate([jnp.where(hit, high[g:g + 1], 0.0), jnp.where(hit, low[g:g + 1], 0.0)], axis=0)
            acc = acc + exact_dot(lhs, ones_where(lane_of[:, g:g + 1] == c))
        found = (acc[:GROUPS] * 256.0 + acc[GROUPS:]).astype(jnp.int32)
        found_ref[pl.ds(b * GROUPS, GROUPS), :] = found
        return found

    early_groups = 2 * EARLY // 128
    firsts = [find(b)[:early_groups] for b in (1, 3)]
    for i, first in enumerate(firsts):
        slab_no[pl.ds(i * early_groups, early_groups), :] = lax.shift_right_logical(first, 3)
    to_smem = pltpu.make_async_copy(slab_no, slab_no_smem, meta_sem)
    to_smem.start()
    for i, first in enumerate(firsts):
        row_of = to_column(eye, first & 7)
        for g in range(early_groups):
            picks[pl.ds((i * early_groups + g) * 128, 128), :] = jnp.broadcast_to(row_of[:, g:g + 1], (128, 128))
    to_smem.wait()

    n = EARLY // TILE
    for i in range(2):
        for t in range(n):
            at = core * EARLY + t * TILE
            fetch_slabs(
                table_ref, lambda group, lane: slab_no_smem[group, lane],
                i * early_groups + lax.div(at, 128), lax.rem(at, 128), slabs, i * n + t, slab_sem,
            )
    for b in (0, 2):
        find(b)
    outs = []
    for i in range(2):
        for t in range(n):
            step = i * n + t
            base = pl.multiple_of(i * early_groups * 128 + core * EARLY + t * TILE, TILE)
            pick_rows(picks, base, slabs, step, slab_sem, rows, step)
            target = (part_ref, mine_ref)[i]
            outs.append(pltpu.make_async_copy(rows.at[step], target.at[pl.ds(t * TILE, TILE), :], row_sem.at[step]))
            outs[-1].start()
    for copy in outs:
        copy.wait()


def early_rows(token_ids, table):
    n_ids, (slab_count, _, dim) = token_ids.shape[0], table.shape
    groups, steps = n_ids // 128, 2 * EARLY // TILE
    any_spec, vmem = pl.BlockSpec(memory_space=pl.ANY), pl.BlockSpec(memory_space=pltpu.VMEM)
    rows = jax.ShapeDtypeStruct((EARLY, dim), jnp.bfloat16)
    return pl.pallas_call(
        functools.partial(early_kernel, 8 * slab_count),
        out_shape=[
            rows, rows,
            jax.ShapeDtypeStruct((4 * GROUPS, 128), jnp.int32),
            jax.ShapeDtypeStruct((2, groups // 2, 128), jnp.float32),
            jax.ShapeDtypeStruct((8, 128), jnp.int32),
            jax.ShapeDtypeStruct((1, 128), jnp.int32),
        ],
        in_specs=[vmem, any_spec],
        out_specs=[any_spec, any_spec, vmem, vmem, vmem, vmem],
        scratch_shapes=[
            pltpu.VMEM((8, 128), jnp.int32),
            pltpu.SMEM((8, 128), jnp.int32),
            pltpu.VMEM((4 * EARLY, 128), jnp.int32),
            pltpu.VMEM((steps, 8 * TILE, dim), jnp.bfloat16),
            pltpu.VMEM((steps, TILE, dim), jnp.bfloat16),
            pltpu.SemaphoreType.DMA,
            pltpu.SemaphoreType.DMA((steps,)),
            pltpu.SemaphoreType.DMA((steps,)),
        ],
        compiler_params=pltpu.CompilerParams(vmem_limit_bytes=40 << 20),
        cost_estimate=pl.CostEstimate(flops=1 << 32, bytes_accessed=1 << 25, transcendentals=0),
        name="early_rows",
    )(token_ids.reshape(groups, 128), table)


def gather_kernel(
    found_ref, counts_ref, found_vmem, need_in, table_ref, out_ref, need_ref, picks, slabs, rows, steps, slab_sem, row_sem,
):
    need_ref[...] = need_in[...]
    core = lax.rem(lax.axis_index("tp"), 2)
    eye = ones_where(
        lax.broadcasted_iota(jnp.int32, (128, 128), 0) == lax.broadcasted_iota(jnp.int32, (128, 128), 1)
    )
    row_of = to_column(eye, found_vmem[...] & 7)
    per_block = out_ref.shape[0] // 4
    for b in range(4):
        for g in range(per_block // 128):
            picks[pl.ds(b * per_block + g * 128, 128), :] = jnp.broadcast_to(
                row_of[:, b * GROUPS + g:b * GROUPS + g + 1], (128, 128)
            )

    tiles = per_block // TILE
    n_steps = 0
    for b in (1, 3, 0, 2):
        rest0, rest1 = counts_ref[b, 0], counts_ref[4 + b, 0]
        start = jnp.where(core == 0, 2 * EARLY, 2 * EARLY + rest0)
        end = jnp.where(core == 0, 2 * EARLY + rest0, 2 * EARLY + rest0 + rest1)
        if b % 2 == 0:
            for t in range(EARLY // TILE):
                steps[n_steps + t] = b * tiles + core * (EARLY // TILE) + t
            n_steps = n_steps + EARLY // TILE
        first = lax.div(start, TILE)
        last = jnp.where(end > start, lax.div(end + TILE - 1, TILE), first)

        def note(t, _, b=b, first=first, n_steps=n_steps):
            steps[n_steps + t - first] = b * tiles + t
            return 0

        lax.fori_loop(first, last, note, 0)
        n_steps = n_steps + last - first

    def fetch(step):
        tile = steps[step]
        at = lax.rem(tile, tiles) * TILE
        group = lax.div(tile, tiles) * GROUPS + lax.div(at, 128)
        fetch_slabs(
            table_ref, lambda g, lane: lax.shift_right_logical(found_ref[g, lane], 3),
            group, lax.rem(at, 128), slabs, lax.rem(step, SLOTS), slab_sem,
        )

    def first_fetch(step, _):
        fetch(step)
        return 0

    lax.fori_loop(0, jnp.minimum(n_steps, SLOTS - 1), first_fetch, 0)

    def out_copy(step):
        slot = lax.rem(step, 2)
        return pltpu.make_async_copy(
            rows.at[slot], out_ref.at[pl.ds(steps[step] * TILE, TILE), :], row_sem.at[slot]
        )

    def work(step, _):
        @pl.when(step + SLOTS - 1 < n_steps)
        def _():
            fetch(step + SLOTS - 1)

        @pl.when(step >= 2)
        def _():
            out_copy(step - 2).wait()

        base = pl.multiple_of(steps[step] * TILE, TILE)
        pick_rows(picks, base, slabs, lax.rem(step, SLOTS), slab_sem, rows, lax.rem(step, 2))
        out_copy(step).start()
        return 0

    lax.fori_loop(0, n_steps, work, 0)
    for back in (2, 1):
        @pl.when(n_steps >= back)
        def _(back=back):
            out_copy(n_steps - back).wait()


def gather_rows(found, counts, need, table, per_block):
    dim = table.shape[2]
    smem, vmem = pl.BlockSpec(memory_space=pltpu.SMEM), pl.BlockSpec(memory_space=pltpu.VMEM)
    return pl.pallas_call(
        gather_kernel,
        out_shape=[
            jax.ShapeDtypeStruct((4 * per_block, dim), jnp.bfloat16),
            jax.ShapeDtypeStruct(need.shape, need.dtype),
        ],
        in_specs=[smem, smem, vmem, vmem, pl.BlockSpec(memory_space=pl.ANY)],
        out_specs=[pl.BlockSpec(memory_space=pl.ANY), vmem],
        scratch_shapes=[
            pltpu.VMEM((4 * per_block, 128), jnp.int32),
            pltpu.VMEM((SLOTS, 8 * TILE, dim), jnp.bfloat16),
            pltpu.VMEM((2, TILE, dim), jnp.bfloat16),
            pltpu.SMEM((4 * per_block // TILE,), jnp.int32),
            pltpu.SemaphoreType.DMA((SLOTS,)),
            pltpu.SemaphoreType.DMA((2,)),
        ],
        compiler_params=pltpu.CompilerParams(vmem_limit_bytes=40 << 20),
        cost_estimate=pl.CostEstimate(flops=1 << 34, bytes_accessed=1 << 26, transcendentals=0),
        name="gather_rows",
    )(found, counts, found, need, table)


def merge_into(mine_ref, theirs_ref, at, n, place, rest0, rest1, core):
    core0_end = 2 * EARLY + rest0
    chip_end = core0_end + rest1
    dim = mine_ref.shape[1]

    @pl.loop(0, n // 16)
    def _(t):
        span = pl.ds(pl.multiple_of(at + t * 16, 16), 16)
        pos = place + t * 16 + lax.broadcasted_iota(jnp.int32, (16, dim), 0)
        from_core0 = pos < core0_end
        if place < 2 * EARLY:
            from_core0 = (pos < EARLY) | ((pos >= 2 * EARLY) & from_core0)
        merged = jnp.where(
            jnp.where(from_core0, 0, 1) == core,
            mine_ref[span, :].astype(jnp.float32), theirs_ref[span, :].astype(jnp.float32),
        )
        mine_ref[span, :] = jnp.where(pos < chip_end, merged, 0.0).astype(jnp.bfloat16)


def merge_kernel(stride, counts_ref, rows_ref, out_ref, mine, theirs, send, recv, load_sem, out_sem):
    me, dp = lax.axis_index("tp"), lax.axis_index("dp")
    core = lax.rem(me, 2)
    partner = me + 1 - 2 * core
    barrier = pltpu.get_barrier_semaphore()
    pl.semaphore_signal(barrier, inc=1, device_id=(dp, partner), device_id_type=MESH)
    n, ways = mine.shape[0], send.shape[0]
    size = n // ways
    loads = [
        pltpu.make_async_copy(
            rows_ref.at[pl.ds(3 * stride + 2 * EARLY + i * size, size), :], mine.at[pl.ds(i * size, size), :],
            load_sem.at[i],
        )
        for i in range(ways)
    ]
    for copy in loads:
        copy.start()
    pl.semaphore_wait(barrier, 1)
    pair = [
        pltpu.make_async_remote_copy(
            src_ref=rows_ref.at[pl.ds(stride + 2 * EARLY + i * size, size), :],
            dst_ref=theirs.at[pl.ds(i * size, size), :],
            send_sem=send.at[i], recv_sem=recv.at[i], device_id=(dp, partner), device_id_type=MESH,
        )
        for i in range(ways)
    ]
    outs = [
        pltpu.make_async_copy(
            mine.at[pl.ds(i * size, size), :], out_ref.at[pl.ds(i * size, size), :], out_sem.at[i]
        )
        for i in range(ways)
    ]
    for copy in pair:
        copy.start()
    for i in range(ways):
        loads[i].wait()
        pair[i].wait_recv()
        merge_into(mine, theirs, i * size, size, 2 * EARLY + i * size, counts_ref[3, 0], counts_ref[7, 0], core)
        outs[i].start()
    for copy in outs:
        copy.wait()
    for copy in pair:
        copy.wait_send()


def merge_rows(counts, rows):
    n, dim, ways = max(PACKED) - 2 * EARLY, rows.shape[1], 4
    dma = pltpu.SemaphoreType.DMA
    return pl.pallas_call(
        functools.partial(merge_kernel, rows.shape[0] // 4),
        out_shape=jax.ShapeDtypeStruct((n, dim), jnp.bfloat16),
        in_specs=[pl.BlockSpec(memory_space=pltpu.SMEM), pl.BlockSpec(memory_space=pl.ANY)],
        out_specs=pl.BlockSpec(memory_space=pl.ANY),
        scratch_shapes=[pltpu.VMEM((n, dim), jnp.bfloat16)] * 2 + [dma((ways,))] * 4,
        compiler_params=pltpu.CompilerParams(
            collective_id=len(PACKED) + 1, has_side_effects=True, vmem_limit_bytes=16 << 20
        ),
        cost_estimate=pl.CostEstimate(flops=1 << 30, bytes_accessed=1 << 23, transcendentals=0),
        name="merge_rows",
    )(counts, rows)


def block_kernel(
    cap, stride, parts, gain_ref, place_ref, counts_ref, part_ref, mine_ref, near_ref, far_ref, merged_ref, rows_ref, w1_ref, w2_ref,
    out_ref, w1p_ref, w2p_ref, sums_ref,
    inbox, ours_rows, normed, kept, acc, w1_buf, w2_buf, sum_buf, out_buf,
    pair_send, pair_recv, load_sem, w_send, w_recv, ready, x_send, x_recv, w_sem, s_send, s_recv, r_sem, o_sem, early_sem,
):
    me, dp = lax.axis_index("tp"), lax.axis_index("dp")
    core = lax.rem(me, 2)
    partner = me + 1 - 2 * core
    other = lax.rem(me + 2, 4)
    dim = w1_ref.shape[0]
    n_tok = out_ref.shape[0]
    width = w1_ref.shape[1]
    w_steps = width // WIDTH
    n_chunks = n_tok // CHUNK
    n_pieces = n_tok // PIECE

    barrier = pltpu.get_barrier_semaphore()
    for peer in (partner, other):
        pl.semaphore_signal(barrier, inc=1, device_id=(dp, peer), device_id_type=MESH)
    pl.semaphore_wait(barrier, 2)

    def remote(src, dst, send, recv, peer):
        return pltpu.make_async_remote_copy(
            src_ref=src, dst_ref=dst, send_sem=send, recv_sem=recv, device_id=(dp, peer), device_id_type=MESH
        )

    own_zone = pl.ds(pl.multiple_of(core * EARLY, EARLY), EARLY)
    partner_zone = pl.ds(pl.multiple_of((1 - core) * EARLY, EARLY), EARLY)

    def pair(i, p, at, n):
        src = pl.ds((1 - p) * stride + at, n)
        return remote(rows_ref.at[src, :], inbox.at[p, pl.ds(at, n), :], pair_send.at[i], pair_recv.at[i], partner)

    def load(i, p, at, n):
        src = pl.ds((3 - p) * stride + at, n)
        return pltpu.make_async_copy(rows_ref.at[src, :], ours_rows.at[1 - p, pl.ds(at, n), :], load_sem.at[i])

    def cross(i, p, at, n):
        span = pl.ds(at, n)
        return remote(ours_rows.at[1 - p, span, :], inbox.at[p, span, :], x_send.at[i], x_recv.at[i], other)

    pair_early = remote(part_ref, inbox.at[0, own_zone, :], early_sem.at[0], early_sem.at[1], partner)
    load_early = pltpu.make_async_copy(mine_ref, ours_rows.at[1, own_zone, :], early_sem.at[2])
    take_early = [
        pltpu.make_async_copy(near_ref, inbox.at[0, own_zone, :], early_sem.at[3]),
        pltpu.make_async_copy(far_ref, inbox.at[0, partner_zone, :], early_sem.at[4]),
    ]

    weights = [
        remote(w1_ref, w1p_ref, w_send.at[0], w_recv.at[0], partner),
        remote(w2_ref, w2p_ref, w_send.at[1], w_recv.at[1], partner),
    ]
    late = cap - 2 * EARLY
    late_zone = pl.ds(2 * EARLY, late)
    late_cross = remote(
        merged_ref.at[pl.ds(0, late), :], inbox.at[0, late_zone, :], early_sem.at[5], early_sem.at[6], other
    ) if cap < stride else None
    late_load = pltpu.make_async_copy(
        merged_ref.at[pl.ds(0, late), :], ours_rows.at[1, late_zone, :], early_sem.at[7]
    ) if cap < stride else None
    if late_cross is not None:
        late_cross.start()
    for i, part in enumerate(parts):
        pair(i, *part).start()
        load(i, *part).start()
    if late_load is not None:
        late_load.start()
    pair_early.start()
    load_early.start()
    for copy in weights:
        copy.start()

    def fetch_weights(step, slot, start):
        @pl.when(step < w_steps)
        def _():
            cols = pl.ds(pl.multiple_of(step * WIDTH, WIDTH), WIDTH)
            start(pltpu.make_async_copy(w1_ref.at[:, cols], w1_buf.at[slot], w_sem.at[0, slot]))
            start(pltpu.make_async_copy(w2_ref.at[cols, :], w2_buf.at[slot], w_sem.at[1, slot]))

        @pl.when(step >= w_steps)
        def _():
            cols = pl.ds(pl.multiple_of((step - w_steps) * WIDTH, WIDTH), WIDTH)
            start(pltpu.make_async_copy(w1p_ref.at[:, cols], w1_buf.at[slot], w_sem.at[0, slot]))
            start(pltpu.make_async_copy(w2p_ref.at[cols, :], w2_buf.at[slot], w_sem.at[1, slot]))

    fetch_weights(0, 0, lambda copy: copy.start())

    def merge(p, at, n):
        b = 1 - p
        merge_into(
            ours_rows.at[b], inbox.at[p], at, n, at, counts_ref[2 + b, 0], counts_ref[6 + b, 0], core
        )

    for i, part in enumerate(parts):
        load(i, *part).wait()
        pair(i, *part).wait_recv()
        merge(*part)
        pl.semaphore_signal(ready.at[i], inc=1, device_id=(dp, other), device_id_type=MESH)
        pl.semaphore_wait(ready.at[i], 1)
        cross(i, *part).start()
    load_early.wait()
    pair_early.wait_recv()
    merge(0, 0, 2 * EARLY)
    for copy in take_early:
        copy.start()
    for copy in take_early:
        copy.wait()
    if late_load is not None:
        late_load.wait()

    gain_rows = gain_ref[...].astype(jnp.float32)
    gain = jnp.concatenate([gain_rows[i:i + 1] for i in range(gain_ref.shape[0])], axis=1)

    sums_land = sum_buf if cap < stride else sums_ref

    def send_sums(piece):
        span = pl.ds(pl.multiple_of(piece * PIECE, PIECE), PIECE)
        return remote(acc.at[span, :], sums_land.at[span, :], s_send.at[piece], s_recv.at[piece], other)

    @pl.loop(0, 2)
    def _(b):
        for p in range(2):
            @pl.when(b == p)
            def _(p=p):
                if p == 0 and late_cross is not None:
                    late_cross.wait_recv()
                for i, part in enumerate(parts):
                    if part[0] == p:
                        cross(i, *part).wait_recv()

        @pl.loop(0, n_tok // 256)
        def _(t):
            span = pl.ds(pl.multiple_of(t * 256, 256), 256)
            slot = lax.broadcasted_iota(jnp.int32, (128, cap), 1).astype(jnp.float32)
            diagonal = lax.broadcasted_iota(jnp.int32, (128, 128), 0) == lax.broadcasted_iota(
                jnp.int32, (128, 128), 1
            )

            def pick_from(side):
                picks = []
                for g in range(2):
                    row = place_ref[side, pl.ds(b * (n_tok // 128) + 2 * t + g, 1), :]
                    column = jnp.sum(jnp.where(diagonal, row, 0.0), axis=1, keepdims=True)
                    picks.append(ones_where(slot == column))
                return jnp.concatenate(picks, axis=0)

            pick_ours, pick_other = pick_from(0), pick_from(1)
            rows = jnp.dot(pick_ours, ours_rows[b], preferred_element_type=jnp.float32) + jnp.dot(
                pick_other, inbox[b], preferred_element_type=jnp.float32
            )
            kept[span, :] = rows.astype(jnp.bfloat16)
            inv_rms = lax.rsqrt(jnp.mean(rows * rows, axis=-1, keepdims=True) + RMS_EPS)
            normed[span, :] = (rows * inv_rms * gain).astype(jnp.bfloat16)

        @pl.loop(0, n_chunks)
        def _(chunk):
            tok = pl.ds(pl.multiple_of(chunk * CHUNK, CHUNK), CHUNK)
            out_rows = pl.ds(pl.multiple_of(b * n_tok + chunk * CHUNK, CHUNK), CHUNK)
            acc[out_rows, :] = jnp.zeros((CHUNK, dim), jnp.float32)

            @pl.loop(0, 2 * w_steps)
            def _(w):
                step = (b * n_chunks + chunk) * 2 * w_steps + w
                slot = lax.rem(step, 2)
                fetch_weights(w, slot, lambda copy: copy.wait())

                @pl.when(step == w_steps - 1)
                def _():
                    for copy in weights:
                        copy.wait_recv()

                @pl.when(step + 1 < 2 * n_chunks * 2 * w_steps)
                def _():
                    fetch_weights(lax.rem(step + 1, 2 * w_steps), 1 - slot, lambda copy: copy.start())

                parts = []
                for half in range(2):
                    cols = pl.ds(half * (WIDTH // 2), WIDTH // 2)
                    z = jnp.dot(normed[tok, :], w1_buf[slot, :, cols], preferred_element_type=jnp.float32)
                    z = z.astype(jnp.bfloat16).astype(jnp.float32)
                    inner = 0.7978845608028654 * (z + 0.044715 * (z * z * z))
                    parts.append((0.5 * z * (1.0 + jnp.tanh(inner))).astype(jnp.bfloat16))
                hidden = jnp.concatenate(parts, axis=1)
                for half in range(2):
                    cols = pl.ds(half * (dim // 2), dim // 2)
                    acc[out_rows, cols] += jnp.dot(
                        hidden, w2_buf[slot, :, cols], preferred_element_type=jnp.float32
                    )

            @pl.when(b == 0)
            def _():
                for q in range(CHUNK // PIECE):
                    send_sums(chunk * (CHUNK // PIECE) + q).start()

    sums_in_vmem = cap < stride

    def take_sums(piece, slot):
        span = pl.ds(pl.multiple_of(piece * PIECE, PIECE), PIECE)
        return pltpu.make_async_copy(sums_ref.at[span, :], sum_buf.at[slot], r_sem.at[slot])

    def put_out(piece, slot):
        span = pl.ds(pl.multiple_of(piece * PIECE, PIECE), PIECE)
        return pltpu.make_async_copy(out_buf.at[slot], out_ref.at[span, :], o_sem.at[slot])

    @pl.loop(0, n_pieces)
    def _(piece):
        slot = lax.rem(piece, 2)
        send_sums(piece).wait_recv()
        if not sums_in_vmem:
            take = take_sums(piece, slot)
            take.start()
            take.wait()

        @pl.when(piece >= 2)
        def _():
            put_out(piece - 2, slot).wait()

        span = pl.ds(pl.multiple_of(piece * PIECE, PIECE), PIECE)
        own = pl.ds(pl.multiple_of(n_tok + piece * PIECE, PIECE), PIECE)
        total = acc[own, :] + (sums_land[span, :] if sums_in_vmem else sum_buf[slot])
        out_buf[slot] = (kept[span, :].astype(jnp.float32) + total).astype(jnp.bfloat16)
        put_out(piece, slot).start()

    put_out(n_pieces - 2, lax.rem(n_pieces - 2, 2)).wait()
    put_out(n_pieces - 1, lax.rem(n_pieces - 1, 2)).wait()

    sent = [pair(i, *part) for i, part in enumerate(parts)] + [cross(i, *part) for i, part in enumerate(parts)]
    if late_cross is not None:
        sent.append(late_cross)
    for copy in [pair_early] + sent + weights:
        copy.wait_send()

    @pl.loop(0, n_pieces)
    def _(piece):
        send_sums(piece).wait_send()


def split_rows(p, first, last, ways=4):
    cuts = [first + 16 * ((last - first) // 16 * i // ways) for i in range(ways + 1)]
    return [(p, cuts[i], cuts[i + 1] - cuts[i]) for i in range(ways)]


def mlp_block(packed, collective_id, gain, place, counts, part, mine, near, far, merged, rows, w_in, w_out):
    n_tok = place.shape[1] * 64
    stride = rows.shape[0] // 4
    cap = packed or stride
    parts = ([] if packed else split_rows(0, 2 * EARLY, cap)) + split_rows(1, 0, cap)
    n_parts = len(parts)
    dim, width = w_in.shape
    any_spec, vmem = pl.BlockSpec(memory_space=pl.ANY), pl.BlockSpec(memory_space=pltpu.VMEM)
    smem = pl.BlockSpec(memory_space=pltpu.SMEM)
    dma = pltpu.SemaphoreType.DMA
    n_pieces = n_tok // PIECE
    flops = 2 * (2 * n_tok) * dim * (2 * width) * 2
    return pl.pallas_call(
        functools.partial(block_kernel, cap, stride, parts),
        out_shape=[
            jax.ShapeDtypeStruct((n_tok, dim), jnp.bfloat16),
            jax.ShapeDtypeStruct(w_in.shape, w_in.dtype),
            jax.ShapeDtypeStruct(w_out.shape, w_out.dtype),
            jax.ShapeDtypeStruct((8 if packed else n_tok, dim), jnp.float32),
        ],
        in_specs=[vmem, vmem, smem] + [any_spec] * 8,
        out_specs=[any_spec] * 4,
        scratch_shapes=[
            pltpu.VMEM((2, cap, dim), jnp.bfloat16),
            pltpu.VMEM((2, cap, dim), jnp.bfloat16),
            pltpu.VMEM((n_tok, dim), jnp.bfloat16),
            pltpu.VMEM((n_tok, dim), jnp.bfloat16),
            pltpu.VMEM((2 * n_tok, dim), jnp.float32),
            pltpu.VMEM((2, dim, WIDTH), jnp.bfloat16),
            pltpu.VMEM((2, WIDTH, dim), jnp.bfloat16),
            pltpu.VMEM((n_tok, dim) if packed else (2, PIECE, dim), jnp.float32),
            pltpu.VMEM((2, PIECE, dim), jnp.bfloat16),
            dma((n_parts,)), dma((n_parts,)), dma((n_parts,)), dma((2,)), dma((2,)),
            pltpu.SemaphoreType.REGULAR((n_parts,)),
            dma((n_parts,)), dma((n_parts,)), dma((2, 2)), dma((n_pieces,)), dma((n_pieces,)), dma((2,)), dma((2,)), dma((8,)),
        ],
        compiler_params=pltpu.CompilerParams(
            collective_id=collective_id, has_side_effects=True, vmem_limit_bytes=67043328
        ),
        cost_estimate=pl.CostEstimate(flops=flops, bytes_accessed=1 << 28, transcendentals=0),
        name="mlp_block",
    )(gain, place, counts, part, mine, near, far, merged, rows, w_in, w_out)[0]


def copy_kernel(src_ref, dst_ref, buf, in_sem, out_sem):
    n = buf.shape[0]
    rows = buf.shape[1]
    ins = [pltpu.make_async_copy(src_ref.at[pl.ds(i * rows, rows), :], buf.at[i], in_sem.at[i]) for i in range(n)]
    outs = [pltpu.make_async_copy(buf.at[i], dst_ref.at[pl.ds(i * rows, rows), :], out_sem.at[i]) for i in range(n)]
    for copy in ins:
        copy.start()
    for i in range(n):
        ins[i].wait()
        outs[i].start()
    for copy in outs:
        copy.wait()


def copy_out(x):
    n = 8
    return pl.pallas_call(
        copy_kernel,
        out_shape=jax.ShapeDtypeStruct(x.shape, x.dtype),
        in_specs=[pl.BlockSpec(memory_space=pl.ANY)],
        out_specs=pl.BlockSpec(memory_space=pl.ANY),
        scratch_shapes=[
            pltpu.VMEM((n, x.shape[0] // n, x.shape[1]), x.dtype),
            pltpu.SemaphoreType.DMA((n,)),
            pltpu.SemaphoreType.DMA((n,)),
        ],
        compiler_params=pltpu.CompilerParams(vmem_limit_bytes=62 << 20),
        name="copy_out",
    )(x)


def solution(mesh):
    swap = [(0, 1), (1, 0)]
    near_pairs = [(r, r ^ 2) for r in range(4)]
    far_pairs = [(r, r ^ 3) for r in range(4)]

    def device_step(token_ids, table_shard, norm_gain, w_in_shard, w_out_shard):
        shard_rows, dim = table_shard.shape
        n_tok = token_ids.shape[0] // 4
        table = table_shard.reshape(-1, 8, dim)
        part, mine, found, place, counts, need = early_rows(token_ids, table)
        near = lax.ppermute(mine, "tp", near_pairs)
        far = lax.ppermute(part, "tp", far_pairs)
        rows, need = gather_rows(found, counts, need, table, -(-(n_tok + EARLY) // 128) * 128)
        merged = merge_rows(counts, rows)
        need = jnp.maximum(need, lax.ppermute(need, "dp", swap))[0, 0]
        out = lax.switch(
            sum((need > cap).astype(jnp.int32) for cap in PACKED),
            [functools.partial(mlp_block, cap, i) for i, cap in enumerate(PACKED + (None,))],
            norm_gain.reshape(-1, 128), place, counts, part, mine, near, far, merged, rows, w_in_shard, w_out_shard,
        )
        return copy_out(out)

    return jax.shard_map(
        device_step,
        mesh=mesh,
        in_specs=(P("dp"), P("tp", None), P(), P(None, "tp"), P("tp", None)),
        out_specs=P(("dp", "tp"), None),
        check_vma=False,
    )
```

```python
import functools

import jax
import jax.numpy as jnp
from jax import lax
from jax.experimental import pallas as pl
from jax.experimental.pallas import tpu as pltpu
from jax.sharding import PartitionSpec as P


RMS_EPS = 1e-6
TILE = 64
BATCH = 16
PICK = 32
SLOTS = 5
EARLY = 192
GROUPS = 16
LANES = 128
PIECE = 128
CHUNK = 512
WIDTH = 512
PACKED = (672, 704)
MESH = pl.DeviceIdType.MESH


def ones_where(cond):
    return jnp.where(cond, 1.0, 0.0).astype(jnp.bfloat16)


def exact_dot(lhs, rhs):
    return jnp.dot(lhs.astype(jnp.bfloat16), rhs.astype(jnp.bfloat16), preferred_element_type=jnp.float32)


def fetch_slabs(table_ref, slab_id, slabs, slot, sem, batches=None):
    def batch(k):
        for j in range(k * BATCH, (k + 1) * BATCH):
            pltpu.make_async_copy(
                table_ref.at[slab_id(j)], slabs.at[slot, pl.ds(8 * j, 8), :], sem.at[slot]
            ).start()

    for k in range(TILE // BATCH):
        if batches is None:
            batch(k)
        else:
            pl.when(batches(k))(functools.partial(batch, k))


def wait_slabs(slabs, slot, sem, batches=None):
    def wait(n):
        some = slabs.at[slot, pl.ds(0, 8 * n), :]
        pltpu.make_async_copy(some, some, sem.at[slot]).wait()

    if batches is None:
        wait(TILE)
    else:
        for k in range(TILE // BATCH):
            pl.when(batches(k))(functools.partial(wait, BATCH))


def pick_rows(picks, base, slabs, slot, rows, row_slot):
    col = lax.broadcasted_iota(jnp.int32, (PICK, 8 * PICK), 1)
    first_col = 8 * lax.broadcasted_iota(jnp.int32, (PICK, 8 * PICK), 0)
    for part in range(TILE // PICK):
        pick = picks[pl.ds(base + part * PICK, PICK), :]
        want = jnp.concatenate([pick] * (8 * PICK // LANES), axis=1) + first_col
        rows[row_slot, pl.ds(part * PICK, PICK), :] = exact_dot(
            ones_where(col == want), slabs[slot, pl.ds(part * 8 * PICK, 8 * PICK), :]
        ).astype(jnp.bfloat16)


def to_column(eye, values):
    return lax.dot_general(
        eye, values.astype(jnp.float32).astype(jnp.bfloat16), (((1,), (1,)), ((), ())),
        preferred_element_type=jnp.float32,
    ).astype(jnp.int32)


def early_kernel(
    shard_rows, tokens_ref, table_ref, mine_ref, found_ref, place_ref, counts_ref, need_ref,
    list_ref, slab_no, slab_no_smem, meta_sem, picks, slabs, rows, slab_sem, row_sem,
):
    me = lax.axis_index("tp")
    chip, core = lax.div(me, 2), lax.rem(me, 2)
    partner, other = me + 1 - 2 * core, lax.rem(me + 2, 4)
    other_partner = other + 1 - 2 * core
    blocks = [other_partner, partner, other, me]
    groups = tokens_ref.shape[0]
    per = groups // 4

    ids = jnp.concatenate([tokens_ref[pl.ds(pl.multiple_of(b * per, per), per), :] for b in blocks], axis=0)
    owner = sum((ids >= q * shard_rows).astype(jnp.int32) for q in (1, 2, 3))
    mask = jnp.concatenate([jnp.where(owner == q, 1.0, 0.0) for q in range(4)], axis=0).astype(jnp.bfloat16)
    r = lax.broadcasted_iota(jnp.int32, (LANES, LANES), 0)
    c = lax.broadcasted_iota(jnp.int32, (LANES, LANES), 1)
    same = lax.div(r, per) == lax.div(c, per)
    ones = jnp.ones((LANES, LANES), jnp.bfloat16)
    rank = exact_dot(mask, ones_where(r <= c)) + exact_dot(exact_dot(ones_where(same & (c < r)), mask), ones)
    total = exact_dot(exact_dot(ones_where(same), mask), ones)
    rank = [rank[q * groups:(q + 1) * groups] - 1.0 for q in range(4)]
    rest = [jnp.maximum(total[q * groups:(q + 1) * groups] - EARLY, 0.0) for q in range(4)]

    def placed(q):
        late = EARLY + (rest[q - 1] if q % 2 else 0.0)
        return rank[q] + jnp.where(rank[q] < EARLY, float(EARLY * (q % 2)), late)

    place = jnp.where(owner == 0, placed(0), jnp.where(
        owner == 1, placed(1), jnp.where(owner == 2, placed(2), placed(3))
    )).astype(jnp.int32)
    ours = lax.shift_right_logical(owner, 1) == chip
    place_ref[0] = jnp.where(ours, place, -1)[groups // 2:].astype(jnp.float32)
    place_ref[1] = jnp.where(ours, -1, place)[groups // 2:].astype(jnp.float32)
    for i, rests in enumerate((jnp.where(chip == 0, rest[0], rest[2]), jnp.where(chip == 0, rest[1], rest[3]))):
        for b in range(4):
            counts_ref[pl.ds(4 * i + b, 1), :] = rests[b * per:b * per + 1].astype(jnp.int32)
    need = jnp.max(jnp.maximum(rest[0] + rest[1], rest[2] + rest[3]), axis=0, keepdims=True)
    need_ref[...] = need.astype(jnp.int32) + 2 * EARLY

    mine = owner == me
    local = jnp.where(mine, ids - me * shard_rows, 0)
    high, low = lax.shift_right_logical(local, 8).astype(jnp.float32), (local & 255).astype(jnp.float32)
    place_group = lax.shift_right_logical(place, 7)
    eye = ones_where(r == c)
    lane_of = to_column(eye, place & 127)
    group_row = lax.broadcasted_iota(jnp.int32, (GROUPS, LANES), 0)

    def find(b):
        acc = jnp.zeros((2 * GROUPS, LANES), jnp.float32)
        for g in range(b * per, (b + 1) * per):
            hit = (place_group[g:g + 1] == group_row) & mine[g:g + 1]
            lhs = jnp.concatenate([jnp.where(hit, high[g:g + 1], 0.0), jnp.where(hit, low[g:g + 1], 0.0)], axis=0)
            acc = acc + exact_dot(lhs, ones_where(lane_of[:, g:g + 1] == c))
        found = (acc[:GROUPS] * 256.0 + acc[GROUPS:]).astype(jnp.int32)
        found_ref[pl.ds(b * GROUPS, GROUPS), :] = found
        if b == 1:
            list_ref[...] = found[:8]
        return found

    slab_no[...] = lax.shift_right_logical(find(3)[:8], 3)
    to_smem = pltpu.make_async_copy(slab_no, slab_no_smem, meta_sem)
    to_smem.start()
    to_smem.wait()
    early_picks(eye, found_ref[pl.ds(3 * GROUPS, 8), :], picks)
    gather_early(
        core, lambda group, lane: slab_no_smem[group, lane], table_ref, mine_ref, picks, slabs, rows,
        slab_sem, row_sem, lambda: [find(b) for b in (1, 0, 2)],
    )


def early_picks(eye, found, picks):
    row_of = to_column(eye, found & 7)
    for g in range(2 * EARLY // LANES):
        picks[pl.ds(g * LANES, LANES), :] = jnp.broadcast_to(row_of[:, g:g + 1], (LANES, LANES))


def gather_early(core, slab_id, table_ref, out_ref, picks, slabs, rows, slab_sem, row_sem, meanwhile=lambda: None):
    n = EARLY // TILE
    for t in range(n):
        at = core * EARLY + t * TILE
        group, lane = lax.div(at, LANES), lax.rem(at, LANES)
        fetch_slabs(table_ref, lambda j, group=group, lane=lane: slab_id(group, lane + j), slabs, t, slab_sem)
    meanwhile()
    outs = []
    for t in range(n):
        wait_slabs(slabs, t, slab_sem)
        pick_rows(picks, pl.multiple_of(core * EARLY + t * TILE, TILE), slabs, t, rows, t)
        outs.append(pltpu.make_async_copy(rows.at[t], out_ref.at[pl.ds(t * TILE, TILE), :], row_sem.at[t]))
        outs[-1].start()
    for copy in outs:
        copy.wait()


def part_kernel(list_ref, list_vmem, table_ref, part_ref, picks, slabs, rows, slab_sem, row_sem):
    core = lax.rem(lax.axis_index("tp"), 2)
    eye = ones_where(
        lax.broadcasted_iota(jnp.int32, (LANES, LANES), 0) == lax.broadcasted_iota(jnp.int32, (LANES, LANES), 1)
    )
    early_picks(eye, list_vmem[...], picks)
    gather_early(
        core, lambda group, lane: lax.shift_right_logical(list_ref[group, lane], 3), table_ref, part_ref,
        picks, slabs, rows, slab_sem, row_sem,
    )


def early_scratch(dim):
    steps = EARLY // TILE
    return [
        pltpu.VMEM((2 * EARLY, LANES), jnp.int32),
        pltpu.VMEM((steps, 8 * TILE, dim), jnp.bfloat16),
        pltpu.VMEM((steps, TILE, dim), jnp.bfloat16),
        pltpu.SemaphoreType.DMA((steps,)),
        pltpu.SemaphoreType.DMA((steps,)),
    ]


def part_rows(first_places, table):
    dim = table.shape[2]
    any_spec, vmem = pl.BlockSpec(memory_space=pl.ANY), pl.BlockSpec(memory_space=pltpu.VMEM)
    return pl.pallas_call(
        part_kernel,
        out_shape=jax.ShapeDtypeStruct((EARLY, dim), jnp.bfloat16),
        in_specs=[pl.BlockSpec(memory_space=pltpu.SMEM), vmem, any_spec],
        out_specs=any_spec,
        scratch_shapes=early_scratch(dim),
        compiler_params=pltpu.CompilerParams(vmem_limit_bytes=40 << 20),
        cost_estimate=pl.CostEstimate(flops=1 << 32, bytes_accessed=1 << 24, transcendentals=0),
        name="part_rows",
    )(first_places, first_places, table)


def early_rows(token_ids, table):
    n_ids, (slab_count, _, dim) = token_ids.shape[0], table.shape
    groups = n_ids // LANES
    any_spec, vmem = pl.BlockSpec(memory_space=pl.ANY), pl.BlockSpec(memory_space=pltpu.VMEM)
    return pl.pallas_call(
        functools.partial(early_kernel, 8 * slab_count),
        out_shape=[
            jax.ShapeDtypeStruct((EARLY, dim), jnp.bfloat16),
            jax.ShapeDtypeStruct((4 * GROUPS, LANES), jnp.int32),
            jax.ShapeDtypeStruct((2, groups // 2, LANES), jnp.float32),
            jax.ShapeDtypeStruct((8, LANES), jnp.int32),
            jax.ShapeDtypeStruct((1, LANES), jnp.int32),
            jax.ShapeDtypeStruct((8, LANES), jnp.int32),
        ],
        in_specs=[vmem, any_spec],
        out_specs=[any_spec] + [vmem] * 5,
        scratch_shapes=[
            pltpu.VMEM((8, LANES), jnp.int32),
            pltpu.SMEM((8, LANES), jnp.int32),
            pltpu.SemaphoreType.DMA,
        ] + early_scratch(dim),
        compiler_params=pltpu.CompilerParams(vmem_limit_bytes=40 << 20),
        cost_estimate=pl.CostEstimate(flops=1 << 32, bytes_accessed=1 << 25, transcendentals=0),
        name="early_rows",
    )(token_ids.reshape(groups, LANES), table)


def gather_kernel(
    found_ref, counts_ref, found_vmem, need_in, table_ref, out_ref, need_ref, picks, slabs, rows, steps, spans,
    slab_sem, row_sem,
):
    need_ref[...] = need_in[...]
    core = lax.rem(lax.axis_index("tp"), 2)
    eye = ones_where(
        lax.broadcasted_iota(jnp.int32, (LANES, LANES), 0) == lax.broadcasted_iota(jnp.int32, (LANES, LANES), 1)
    )
    row_of = to_column(eye, found_vmem[...] & 7)
    per_block = out_ref.shape[0] // 4
    for b in range(4):
        for g in range(per_block // LANES):
            picks[pl.ds(b * per_block + g * LANES, LANES), :] = jnp.broadcast_to(
                row_of[:, b * GROUPS + g:b * GROUPS + g + 1], (LANES, LANES)
            )

    tiles = per_block // TILE
    n_steps = 0
    for b in (0, 2):
        for t in range(EARLY // TILE):
            steps[n_steps] = b * tiles + core * (EARLY // TILE) + t
            spans[2 * n_steps], spans[2 * n_steps + 1] = 0, TILE
            n_steps += 1
    for b in (1, 3, 0, 2):
        rest0, rest1 = counts_ref[b, 0], counts_ref[4 + b, 0]
        start = jnp.where(core == 0, 2 * EARLY, 2 * EARLY + rest0)
        end = jnp.where(core == 0, 2 * EARLY + rest0, 2 * EARLY + rest0 + rest1)
        first = lax.div(start, TILE)
        last = jnp.where(end > start, lax.div(end + TILE - 1, TILE), first)

        def note(t, _, b=b, first=first, n_steps=n_steps, start=start, end=end):
            at = n_steps + t - first
            steps[at] = b * tiles + t
            spans[2 * at] = jnp.maximum(start - t * TILE, 0)
            spans[2 * at + 1] = jnp.minimum(end - t * TILE, TILE)
            return 0

        lax.fori_loop(first, last, note, 0)
        n_steps = n_steps + last - first

    def batches(step):
        first, last = spans[2 * step], spans[2 * step + 1]
        return lambda k: (first < (k + 1) * BATCH) & (last > k * BATCH)

    def fetch(step):
        tile = steps[step]
        at = lax.rem(tile, tiles) * TILE
        group, lane = lax.div(tile, tiles) * GROUPS + lax.div(at, LANES), lax.rem(at, LANES)
        fetch_slabs(
            table_ref, lambda j: lax.shift_right_logical(found_ref[group, lane + j], 3),
            slabs, lax.rem(step, SLOTS), slab_sem, batches(step),
        )

    def first_fetch(step, _):
        fetch(step)
        return 0

    lax.fori_loop(0, jnp.minimum(n_steps, SLOTS - 1), first_fetch, 0)

    def out_copy(step):
        slot = lax.rem(step, 2)
        return pltpu.make_async_copy(
            rows.at[slot], out_ref.at[pl.ds(steps[step] * TILE, TILE), :], row_sem.at[slot]
        )

    def work(step, _):
        @pl.when(step + SLOTS - 1 < n_steps)
        def _():
            fetch(step + SLOTS - 1)

        @pl.when(step >= 2)
        def _():
            out_copy(step - 2).wait()

        base = pl.multiple_of(steps[step] * TILE, TILE)
        wait_slabs(slabs, lax.rem(step, SLOTS), slab_sem, batches(step))
        pick_rows(picks, base, slabs, lax.rem(step, SLOTS), rows, lax.rem(step, 2))
        out_copy(step).start()
        return 0

    lax.fori_loop(0, n_steps, work, 0)
    for back in (2, 1):
        @pl.when(n_steps >= back)
        def _(back=back):
            out_copy(n_steps - back).wait()


def gather_rows(found, counts, need, table, per_block):
    dim = table.shape[2]
    smem, vmem = pl.BlockSpec(memory_space=pltpu.SMEM), pl.BlockSpec(memory_space=pltpu.VMEM)
    return pl.pallas_call(
        gather_kernel,
        out_shape=[
            jax.ShapeDtypeStruct((4 * per_block, dim), jnp.bfloat16),
            jax.ShapeDtypeStruct(need.shape, need.dtype),
        ],
        in_specs=[smem, smem, vmem, vmem, pl.BlockSpec(memory_space=pl.ANY)],
        out_specs=[pl.BlockSpec(memory_space=pl.ANY), vmem],
        scratch_shapes=[
            pltpu.VMEM((4 * per_block, LANES), jnp.int32),
            pltpu.VMEM((SLOTS, 8 * TILE, dim), jnp.bfloat16),
            pltpu.VMEM((2, TILE, dim), jnp.bfloat16),
            pltpu.SMEM((4 * per_block // TILE,), jnp.int32),
            pltpu.SMEM((8 * per_block // TILE,), jnp.int32),
            pltpu.SemaphoreType.DMA((SLOTS,)),
            pltpu.SemaphoreType.DMA((2,)),
        ],
        compiler_params=pltpu.CompilerParams(vmem_limit_bytes=40 << 20),
        cost_estimate=pl.CostEstimate(flops=1 << 34, bytes_accessed=1 << 26, transcendentals=0),
        name="gather_rows",
    )(found, counts, found, need, table)


def merge_into(mine_ref, theirs_ref, at, n, place, rest0, rest1, core):
    core0_end = 2 * EARLY + rest0
    chip_end = core0_end + rest1
    dim = mine_ref.shape[1]

    @pl.loop(0, n // 16)
    def _(t):
        span = pl.ds(pl.multiple_of(at + t * 16, 16), 16)
        pos = place + t * 16 + lax.broadcasted_iota(jnp.int32, (16, dim), 0)
        from_core0 = pos < core0_end
        if place < 2 * EARLY:
            from_core0 = (pos < EARLY) | ((pos >= 2 * EARLY) & from_core0)
        merged = jnp.where(
            jnp.where(from_core0, 0, 1) == core,
            mine_ref[span, :].astype(jnp.float32), theirs_ref[span, :].astype(jnp.float32),
        )
        mine_ref[span, :] = jnp.where(pos < chip_end, merged, 0.0).astype(jnp.bfloat16)


def merge_kernel(stride, counts_ref, rows_ref, out_ref, mine, theirs, send, recv, load_sem, out_sem):
    me, dp = lax.axis_index("tp"), lax.axis_index("dp")
    core = lax.rem(me, 2)
    partner = me + 1 - 2 * core
    barrier = pltpu.get_barrier_semaphore()
    pl.semaphore_signal(barrier, inc=1, device_id=(dp, partner), device_id_type=MESH)
    n, ways = mine.shape[0], send.shape[0]
    size = n // ways
    loads = [
        pltpu.make_async_copy(
            rows_ref.at[pl.ds(3 * stride + 2 * EARLY + i * size, size), :], mine.at[pl.ds(i * size, size), :],
            load_sem.at[i],
        )
        for i in range(ways)
    ]
    for copy in loads:
        copy.start()
    pl.semaphore_wait(barrier, 1)
    pair = [
        pltpu.make_async_remote_copy(
            src_ref=rows_ref.at[pl.ds(stride + 2 * EARLY + i * size, size), :],
            dst_ref=theirs.at[pl.ds(i * size, size), :],
            send_sem=send.at[i], recv_sem=recv.at[i], device_id=(dp, partner), device_id_type=MESH,
        )
        for i in range(ways)
    ]
    outs = [
        pltpu.make_async_copy(
            mine.at[pl.ds(i * size, size), :], out_ref.at[pl.ds(i * size, size), :], out_sem.at[i]
        )
        for i in range(ways)
    ]
    for copy in pair:
        copy.start()
    for i in range(ways):
        loads[i].wait()
        pair[i].wait_recv()
        merge_into(mine, theirs, i * size, size, 2 * EARLY + i * size, counts_ref[3, 0], counts_ref[7, 0], core)
        outs[i].start()
    for copy in outs:
        copy.wait()
    for copy in pair:
        copy.wait_send()


def merge_rows(counts, rows):
    n, dim, ways = max(PACKED) - 2 * EARLY, rows.shape[1], 4
    dma = pltpu.SemaphoreType.DMA
    return pl.pallas_call(
        functools.partial(merge_kernel, rows.shape[0] // 4),
        out_shape=jax.ShapeDtypeStruct((n, dim), jnp.bfloat16),
        in_specs=[pl.BlockSpec(memory_space=pltpu.SMEM), pl.BlockSpec(memory_space=pl.ANY)],
        out_specs=pl.BlockSpec(memory_space=pl.ANY),
        scratch_shapes=[pltpu.VMEM((n, dim), jnp.bfloat16)] * 2 + [dma((ways,))] * 4,
        compiler_params=pltpu.CompilerParams(
            collective_id=len(PACKED) + 1, has_side_effects=True, vmem_limit_bytes=16 << 20
        ),
        cost_estimate=pl.CostEstimate(flops=1 << 30, bytes_accessed=1 << 23, transcendentals=0),
        name="merge_rows",
    )(counts, rows)


def block_kernel(
    cap, stride, parts, gain_ref, place_ref, counts_ref, part_ref, mine_ref, near_ref, far_ref, merged_ref, rows_ref, w1_ref, w2_ref,
    out_ref, w1p_ref, w2p_ref, sums_ref,
    inbox, ours_rows, normed, kept, acc, w1_buf, w2_buf, sum_buf, out_buf,
    pair_send, pair_recv, load_sem, w_send, w_recv, ready, x_send, x_recv, w_sem, s_send, s_recv, r_sem, o_sem, early_sem,
):
    me, dp = lax.axis_index("tp"), lax.axis_index("dp")
    core = lax.rem(me, 2)
    partner = me + 1 - 2 * core
    other = lax.rem(me + 2, 4)
    dim = w1_ref.shape[0]
    n_tok = out_ref.shape[0]
    width = w1_ref.shape[1]
    w_steps = width // WIDTH
    n_chunks = n_tok // CHUNK
    n_pieces = n_tok // PIECE

    barrier = pltpu.get_barrier_semaphore()
    for peer in (partner, other):
        pl.semaphore_signal(barrier, inc=1, device_id=(dp, peer), device_id_type=MESH)
    pl.semaphore_wait(barrier, 2)

    def remote(src, dst, send, recv, peer):
        return pltpu.make_async_remote_copy(
            src_ref=src, dst_ref=dst, send_sem=send, recv_sem=recv, device_id=(dp, peer), device_id_type=MESH
        )

    own_zone = pl.ds(pl.multiple_of(core * EARLY, EARLY), EARLY)
    partner_zone = pl.ds(pl.multiple_of((1 - core) * EARLY, EARLY), EARLY)

    def pair(i, p, at, n):
        src = pl.ds((1 - p) * stride + at, n)
        return remote(rows_ref.at[src, :], inbox.at[p, pl.ds(at, n), :], pair_send.at[i], pair_recv.at[i], partner)

    def load(i, p, at, n):
        src = pl.ds((3 - p) * stride + at, n)
        return pltpu.make_async_copy(rows_ref.at[src, :], ours_rows.at[1 - p, pl.ds(at, n), :], load_sem.at[i])

    def cross(i, p, at, n):
        span = pl.ds(at, n)
        return remote(ours_rows.at[1 - p, span, :], inbox.at[p, span, :], x_send.at[i], x_recv.at[i], other)

    pair_early = remote(part_ref, inbox.at[0, own_zone, :], early_sem.at[0], early_sem.at[1], partner)
    load_early = pltpu.make_async_copy(mine_ref, ours_rows.at[1, own_zone, :], early_sem.at[2])
    take_early = [
        pltpu.make_async_copy(near_ref, inbox.at[0, own_zone, :], early_sem.at[3]),
        pltpu.make_async_copy(far_ref, inbox.at[0, partner_zone, :], early_sem.at[4]),
    ]

    weights = [
        remote(w1_ref, w1p_ref, w_send.at[0], w_recv.at[0], partner),
        remote(w2_ref, w2p_ref, w_send.at[1], w_recv.at[1], partner),
    ]
    late = cap - 2 * EARLY
    late_zone = pl.ds(2 * EARLY, late)
    late_cross = remote(
        merged_ref.at[pl.ds(0, late), :], inbox.at[0, late_zone, :], early_sem.at[5], early_sem.at[6], other
    ) if cap < stride else None
    late_load = pltpu.make_async_copy(
        merged_ref.at[pl.ds(0, late), :], ours_rows.at[1, late_zone, :], early_sem.at[7]
    ) if cap < stride else None
    if late_cross is not None:
        late_cross.start()
    for i, part in enumerate(parts):
        pair(i, *part).start()
        load(i, *part).start()
    if late_load is not None:
        late_load.start()
    pair_early.start()
    load_early.start()
    for copy in weights:
        copy.start()

    def fetch_weights(step, slot, start):
        @pl.when(step < w_steps)
        def _():
            cols = pl.ds(pl.multiple_of(step * WIDTH, WIDTH), WIDTH)
            start(pltpu.make_async_copy(w1_ref.at[:, cols], w1_buf.at[slot], w_sem.at[0, slot]))
            start(pltpu.make_async_copy(w2_ref.at[cols, :], w2_buf.at[slot], w_sem.at[1, slot]))

        @pl.when(step >= w_steps)
        def _():
            cols = pl.ds(pl.multiple_of((step - w_steps) * WIDTH, WIDTH), WIDTH)
            start(pltpu.make_async_copy(w1p_ref.at[:, cols], w1_buf.at[slot], w_sem.at[0, slot]))
            start(pltpu.make_async_copy(w2p_ref.at[cols, :], w2_buf.at[slot], w_sem.at[1, slot]))

    fetch_weights(0, 0, lambda copy: copy.start())

    def merge(p, at, n):
        b = 1 - p
        merge_into(
            ours_rows.at[b], inbox.at[p], at, n, at, counts_ref[2 + b, 0], counts_ref[6 + b, 0], core
        )

    for i, part in enumerate(parts):
        load(i, *part).wait()
        pair(i, *part).wait_recv()
        merge(*part)
        pl.semaphore_signal(ready.at[i], inc=1, device_id=(dp, other), device_id_type=MESH)
        pl.semaphore_wait(ready.at[i], 1)
        cross(i, *part).start()
    load_early.wait()
    pair_early.wait_recv()
    merge(0, 0, 2 * EARLY)
    for copy in take_early:
        copy.start()
    for copy in take_early:
        copy.wait()
    if late_load is not None:
        late_load.wait()

    gain_rows = gain_ref[...].astype(jnp.float32)
    gain = jnp.concatenate([gain_rows[i:i + 1] for i in range(gain_ref.shape[0])], axis=1)

    sums_land = sum_buf if cap < stride else sums_ref

    def send_sums(piece):
        span = pl.ds(pl.multiple_of(piece * PIECE, PIECE), PIECE)
        return remote(acc.at[span, :], sums_land.at[span, :], s_send.at[piece], s_recv.at[piece], other)

    @pl.loop(0, 2)
    def _(b):
        for p in range(2):
            @pl.when(b == p)
            def _(p=p):
                if p == 0 and late_cross is not None:
                    late_cross.wait_recv()
                for i, part in enumerate(parts):
                    if part[0] == p:
                        cross(i, *part).wait_recv()

        @pl.loop(0, n_tok // 256)
        def _(t):
            span = pl.ds(pl.multiple_of(t * 256, 256), 256)
            slot = lax.broadcasted_iota(jnp.int32, (LANES, cap), 1).astype(jnp.float32)
            diagonal = lax.broadcasted_iota(jnp.int32, (LANES, LANES), 0) == lax.broadcasted_iota(
                jnp.int32, (LANES, LANES), 1
            )

            def pick_from(side):
                picks = []
                for g in range(2):
                    row = place_ref[side, pl.ds(b * (n_tok // LANES) + 2 * t + g, 1), :]
                    column = jnp.sum(jnp.where(diagonal, row, 0.0), axis=1, keepdims=True)
                    picks.append(ones_where(slot == column))
                return jnp.concatenate(picks, axis=0)

            pick_ours, pick_other = pick_from(0), pick_from(1)
            rows = jnp.dot(pick_ours, ours_rows[b], preferred_element_type=jnp.float32) + jnp.dot(
                pick_other, inbox[b], preferred_element_type=jnp.float32
            )
            kept[span, :] = rows.astype(jnp.bfloat16)
            inv_rms = lax.rsqrt(jnp.mean(rows * rows, axis=-1, keepdims=True) + RMS_EPS)
            normed[span, :] = (rows * inv_rms * gain).astype(jnp.bfloat16)

        @pl.loop(0, n_chunks)
        def _(chunk):
            tok = pl.ds(pl.multiple_of(chunk * CHUNK, CHUNK), CHUNK)
            out_rows = pl.ds(pl.multiple_of(b * n_tok + chunk * CHUNK, CHUNK), CHUNK)
            acc[out_rows, :] = jnp.zeros((CHUNK, dim), jnp.float32)

            @pl.loop(0, 2 * w_steps)
            def _(w):
                step = (b * n_chunks + chunk) * 2 * w_steps + w
                slot = lax.rem(step, 2)
                fetch_weights(w, slot, lambda copy: copy.wait())

                @pl.when(step == w_steps - 1)
                def _():
                    for copy in weights:
                        copy.wait_recv()

                @pl.when(step + 1 < 2 * n_chunks * 2 * w_steps)
                def _():
                    fetch_weights(lax.rem(step + 1, 2 * w_steps), 1 - slot, lambda copy: copy.start())

                parts = []
                for half in range(2):
                    cols = pl.ds(half * (WIDTH // 2), WIDTH // 2)
                    z = jnp.dot(normed[tok, :], w1_buf[slot, :, cols], preferred_element_type=jnp.float32)
                    z = z.astype(jnp.bfloat16).astype(jnp.float32)
                    inner = 0.7978845608028654 * (z + 0.044715 * (z * z * z))
                    parts.append((0.5 * z * (1.0 + jnp.tanh(inner))).astype(jnp.bfloat16))
                hidden = jnp.concatenate(parts, axis=1)
                for half in range(2):
                    cols = pl.ds(half * (dim // 2), dim // 2)
                    acc[out_rows, cols] += jnp.dot(
                        hidden, w2_buf[slot, :, cols], preferred_element_type=jnp.float32
                    )

            @pl.when(b == 0)
            def _():
                for q in range(CHUNK // PIECE):
                    send_sums(chunk * (CHUNK // PIECE) + q).start()

    sums_in_vmem = cap < stride

    def take_sums(piece, slot):
        span = pl.ds(pl.multiple_of(piece * PIECE, PIECE), PIECE)
        return pltpu.make_async_copy(sums_ref.at[span, :], sum_buf.at[slot], r_sem.at[slot])

    def put_out(piece, slot):
        span = pl.ds(pl.multiple_of(piece * PIECE, PIECE), PIECE)
        return pltpu.make_async_copy(out_buf.at[slot], out_ref.at[span, :], o_sem.at[slot])

    @pl.loop(0, n_pieces)
    def _(piece):
        slot = lax.rem(piece, 2)
        send_sums(piece).wait_recv()
        if not sums_in_vmem:
            take = take_sums(piece, slot)
            take.start()
            take.wait()

        @pl.when(piece >= 2)
        def _():
            put_out(piece - 2, slot).wait()

        span = pl.ds(pl.multiple_of(piece * PIECE, PIECE), PIECE)
        own = pl.ds(pl.multiple_of(n_tok + piece * PIECE, PIECE), PIECE)
        total = acc[own, :] + (sums_land[span, :] if sums_in_vmem else sum_buf[slot])
        out_buf[slot] = (kept[span, :].astype(jnp.float32) + total).astype(jnp.bfloat16)
        put_out(piece, slot).start()

    put_out(n_pieces - 2, lax.rem(n_pieces - 2, 2)).wait()
    put_out(n_pieces - 1, lax.rem(n_pieces - 1, 2)).wait()

    sent = [pair(i, *part) for i, part in enumerate(parts)] + [cross(i, *part) for i, part in enumerate(parts)]
    if late_cross is not None:
        sent.append(late_cross)
    for copy in [pair_early] + sent + weights:
        copy.wait_send()

    @pl.loop(0, n_pieces)
    def _(piece):
        send_sums(piece).wait_send()


def split_rows(p, first, last, ways=4):
    cuts = [first + 16 * ((last - first) // 16 * i // ways) for i in range(ways + 1)]
    return [(p, cuts[i], cuts[i + 1] - cuts[i]) for i in range(ways)]


def mlp_block(packed, collective_id, gain, place, counts, part, mine, near, far, merged, rows, w_in, w_out):
    n_tok = place.shape[1] * 64
    stride = rows.shape[0] // 4
    cap = packed or stride
    parts = ([] if packed else split_rows(0, 2 * EARLY, cap)) + split_rows(1, 0, cap)
    n_parts = len(parts)
    dim, width = w_in.shape
    any_spec, vmem = pl.BlockSpec(memory_space=pl.ANY), pl.BlockSpec(memory_space=pltpu.VMEM)
    smem = pl.BlockSpec(memory_space=pltpu.SMEM)
    dma = pltpu.SemaphoreType.DMA
    n_pieces = n_tok // PIECE
    flops = 2 * (2 * n_tok) * dim * (2 * width) * 2
    return pl.pallas_call(
        functools.partial(block_kernel, cap, stride, parts),
        out_shape=[
            jax.ShapeDtypeStruct((n_tok, dim), jnp.bfloat16),
            jax.ShapeDtypeStruct(w_in.shape, w_in.dtype),
            jax.ShapeDtypeStruct(w_out.shape, w_out.dtype),
            jax.ShapeDtypeStruct((8 if packed else n_tok, dim), jnp.float32),
        ],
        in_specs=[vmem, vmem, smem] + [any_spec] * 8,
        out_specs=[any_spec] * 4,
        scratch_shapes=[
            pltpu.VMEM((2, cap, dim), jnp.bfloat16),
            pltpu.VMEM((2, cap, dim), jnp.bfloat16),
            pltpu.VMEM((n_tok, dim), jnp.bfloat16),
            pltpu.VMEM((n_tok, dim), jnp.bfloat16),
            pltpu.VMEM((2 * n_tok, dim), jnp.float32),
            pltpu.VMEM((2, dim, WIDTH), jnp.bfloat16),
            pltpu.VMEM((2, WIDTH, dim), jnp.bfloat16),
            pltpu.VMEM((n_tok, dim) if packed else (2, PIECE, dim), jnp.float32),
            pltpu.VMEM((2, PIECE, dim), jnp.bfloat16),
            dma((n_parts,)), dma((n_parts,)), dma((n_parts,)), dma((2,)), dma((2,)),
            pltpu.SemaphoreType.REGULAR((n_parts,)),
            dma((n_parts,)), dma((n_parts,)), dma((2, 2)), dma((n_pieces,)), dma((n_pieces,)), dma((2,)), dma((2,)), dma((8,)),
        ],
        compiler_params=pltpu.CompilerParams(
            collective_id=collective_id, has_side_effects=True, vmem_limit_bytes=67043328
        ),
        cost_estimate=pl.CostEstimate(flops=flops, bytes_accessed=1 << 28, transcendentals=0),
        name="mlp_block",
    )(gain, place, counts, part, mine, near, far, merged, rows, w_in, w_out)[0]


def copy_kernel(src_ref, dst_ref, buf, in_sem, out_sem):
    n = buf.shape[0]
    rows = buf.shape[1]
    ins = [pltpu.make_async_copy(src_ref.at[pl.ds(i * rows, rows), :], buf.at[i], in_sem.at[i]) for i in range(n)]
    outs = [pltpu.make_async_copy(buf.at[i], dst_ref.at[pl.ds(i * rows, rows), :], out_sem.at[i]) for i in range(n)]
    for copy in ins:
        copy.start()
    for i in range(n):
        ins[i].wait()
        outs[i].start()
    for copy in outs:
        copy.wait()


def copy_out(x):
    n = 4
    return pl.pallas_call(
        copy_kernel,
        out_shape=jax.ShapeDtypeStruct(x.shape, x.dtype),
        in_specs=[pl.BlockSpec(memory_space=pl.ANY)],
        out_specs=pl.BlockSpec(memory_space=pl.ANY),
        scratch_shapes=[
            pltpu.VMEM((n, x.shape[0] // n, x.shape[1]), x.dtype),
            pltpu.SemaphoreType.DMA((n,)),
            pltpu.SemaphoreType.DMA((n,)),
        ],
        compiler_params=pltpu.CompilerParams(vmem_limit_bytes=62 << 20),
        name="copy_out",
    )(x)


def solution(mesh):
    swap = [(0, 1), (1, 0)]
    near_pairs = [(r, r ^ 2) for r in range(4)]
    far_pairs = [(r, r ^ 3) for r in range(4)]

    def device_step(token_ids, table_shard, norm_gain, w_in_shard, w_out_shard):
        _, dim = table_shard.shape
        n_tok = token_ids.shape[0] // 4
        table = table_shard.reshape(-1, 8, dim)
        mine, found, place, counts, need, first_places = early_rows(token_ids, table)
        near = lax.ppermute(mine, "tp", near_pairs)
        part = part_rows(first_places, table)
        far = lax.ppermute(part, "tp", far_pairs)
        rows, need = gather_rows(found, counts, need, table, -(-(n_tok + EARLY) // LANES) * LANES)
        merged = merge_rows(counts, rows)
        need = jnp.maximum(need, lax.ppermute(need, "dp", swap))[0, 0]
        out = lax.switch(
            sum((need > cap).astype(jnp.int32) for cap in PACKED),
            [functools.partial(mlp_block, cap, i) for i, cap in enumerate(PACKED + (None,))],
            norm_gain.reshape(-1, LANES), place, counts, part, mine, near, far, merged, rows, w_in_shard, w_out_shard,
        )
        return copy_out(out)

    return jax.shard_map(
        device_step,
        mesh=mesh,
        in_specs=(P("dp"), P("tp", None), P(), P(None, "tp"), P("tp", None)),
        out_specs=P(("dp", "tp"), None),
        check_vma=False,
    )
```
